8 devices in a mesh: dp: 2 (over y, z), tp: 4 (over x, core).
Axes of the slice: x: 2, y: 2, z: 1, core: 2. Of those that a mesh axis runs over, the one named last changes fastest.
Arguments:
- x: bfloat16 [4096, 2048], P('dp'), parts along dimension 0
- gain: bfloat16 [2048], replicated
- wq: bfloat16 [2048, 4096], P(None, 'tp')
- wk: bfloat16 [2048, 2048], P(None, 'tp')
- wv: bfloat16 [2048, 2048], P(None, 'tp')
- wo: bfloat16 [4096, 2048], P('tp')
Outputs:
- output: bfloat16 [4096, 2048], P('dp'), parts along dimension 0
There are 2 independent parts. The reference program is written for one: setup_inputs(seed, part) draws one part's arguments, and reference() takes and returns one part's arrays. A program takes and returns all parts, laid end to end along the dimension named above; an argument that names none is the same for every part.
All inputs are finite; a program needn't handle non-finite values.
Results may differ from the reference program's by a relative error of at most 0.012.
Values are sent between devices in bfloat16 or wider.
A program may use at most 2 GiB of HBM per device.

```python
import jax
import jax.numpy as jnp
from jax import lax

ROWS = 2048
D = 2048
HEADS = 32
KV_HEADS = 16
HEAD = 128
THETA = 10000


def setup_inputs(seed: int = 0, part: int = 0) -> dict:
    kx, kn, kq, kk, kv, ko = jax.random.split(jax.random.key(seed), 6)

    def weights(key, rows, columns):
        return jax.random.normal(key, (rows, columns), jnp.float32) * rows**-0.5

    drawn = {
        "x": jax.random.normal(jax.random.fold_in(kx, part), (ROWS, D), jnp.float32),
        "gain": 1 + 0.1 * jax.random.normal(kn, (D,), jnp.float32),
        "wq": 2 * weights(kq, D, HEADS * HEAD),
        "wk": 2 * weights(kk, D, KV_HEADS * HEAD),
        "wv": 4 * weights(kv, D, KV_HEADS * HEAD),
        "wo": weights(ko, HEADS * HEAD, D),
    }
    return {k: v.astype(jnp.bfloat16) for k, v in drawn.items()}


def normed(x, gain):
    wide = x.astype(jnp.float32)
    scale = lax.rsqrt(jnp.mean(wide * wide, -1, keepdims=True) + 1e-6)
    return (wide * scale * gain.astype(jnp.float32)).astype(jnp.bfloat16)


def turned(t, place, theta):
    half = t.shape[-1] // 2
    angle = place.astype(jnp.float32)[:, None] * theta ** (-jnp.arange(half, dtype=jnp.float32) / half)
    cos, sin = jnp.cos(angle)[:, None], jnp.sin(angle)[:, None]
    a, b = t[..., :half].astype(jnp.float32), t[..., half:].astype(jnp.float32)
    return jnp.concatenate([a * cos - b * sin, b * cos + a * sin], -1).astype(jnp.bfloat16)


def matmul(a, w):
    return jnp.dot(a, w, preferred_element_type=jnp.float32).astype(jnp.bfloat16)


def einsum(form, a, b):
    return jnp.einsum(form, a.astype(jnp.float32), b.astype(jnp.float32))


def attention(q, k, v):
    scores = einsum("tgsd,ugd->gstu", q, k) * q.shape[-1] ** -0.5
    token = jnp.arange(q.shape[0])
    scores = jnp.where(token[:, None] >= token, scores, -jnp.inf)
    weights = jax.nn.softmax(scores, -1).astype(jnp.bfloat16)
    return einsum("gstu,ugd->tgsd", weights, v).astype(jnp.bfloat16)


def reference(x, gain, wq, wk, wv, wo):
    a, place = normed(x, gain), jnp.arange(ROWS)
    q = turned(matmul(a, wq).reshape(ROWS, HEADS, HEAD), place, THETA).reshape(ROWS, KV_HEADS, -1, HEAD)
    k = turned(matmul(a, wk).reshape(ROWS, KV_HEADS, HEAD), place, THETA)
    v = matmul(a, wv).reshape(ROWS, KV_HEADS, HEAD)
    seen = attention(q, k, v).reshape(ROWS, HEADS * HEAD)
    return (x.astype(jnp.float32) + jnp.dot(seen, wo, preferred_element_type=jnp.float32)).astype(jnp.bfloat16)
```

```python
import functools

import jax
import jax.numpy as jnp
import numpy as np
from jax import lax
from jax.experimental import pallas as pl
from jax.experimental.pallas import tpu as pltpu
from jax.sharding import PartitionSpec as P

HEAD = 128
THETA = 10000
LOG2E = 1.4426950408889634
HIDDEN = -2e30
BQ = 256
PART = 128
EXTRA = 16
F32, BF16 = jnp.float32, jnp.bfloat16
MESH = pl.DeviceIdType.MESH


def _dot(a, b, ca, cb):
    return lax.dot_general(a, b, (((ca,), (cb,)), ((), ())), preferred_element_type=F32)


def _rope_table(rows):
    half = HEAD // 2
    power = np.float32(THETA) ** (-np.arange(half, dtype=np.float32) / np.float32(half))
    angle = np.arange(rows, dtype=np.float32)[:, None] * power.astype(np.float32)
    return np.concatenate([np.cos(angle), np.sin(angle)], -1).astype(np.float32)


def _kernel(gain_ref, x_ref, wq_ref, wk_ref, wv_ref, wo_ref, tab_ref, y_ref,
            x_s, wq_s, wk_s, wv_s, wo_s, tab_s, a_s, q_s, k_s, vt_s, top_s, mix_s, seen_s, sum_s, got_s,
            in_sem, x_sem, wo_sem, seen_send, seen_recv, sum_send, sum_recv, y_send, y_recv):
    rows, d = x_s.shape
    kv = k_s.shape[0]
    wide = seen_s.shape[1] // 2
    half = sum_s.shape[1]
    blocks, parts = rows // BQ, rows // PART
    e = HEAD**-0.5 * LOG2E
    tp = lax.axis_index("tp")
    core = lax.rem(tp, 2)
    partner = {"tp": tp + 1 - 2 * core}
    peer = {"tp": lax.rem(tp + 2, 4)}
    mine = pl.ds(pl.multiple_of(core * half, half), half)
    theirs = pl.ds(pl.multiple_of((1 - core) * half, half), half)

    def at(i, n):
        return pl.ds(pl.multiple_of(i * n, n), n)

    barrier = pltpu.get_barrier_semaphore()
    for other in (partner, peer):
        pl.semaphore_signal(barrier, inc=1, device_id=other, device_id_type=MESH)

    def load_x(i):
        return pltpu.make_async_copy(x_ref.at[at(i, BQ)], x_s.at[at(i, BQ)], x_sem.at[i])

    load_k = pltpu.make_async_copy(wk_ref, wk_s, in_sem.at[0])
    load_v = pltpu.make_async_copy(wv_ref, wv_s, in_sem.at[1])
    load_q = pltpu.make_async_copy(wq_ref, wq_s, in_sem.at[2])
    load_tab = pltpu.make_async_copy(tab_ref, tab_s, in_sem.at[3])
    load_o = pltpu.make_async_copy(wo_ref.at[:, mine], wo_s.at[:wide], in_sem.at[4])
    load_x(0).start()
    load_k.start()
    load_tab.start()
    load_v.start()
    load_q.start()
    load_o.start()

    pl.semaphore_wait(barrier, 2)
    swap_o = pltpu.make_async_remote_copy(
        src_ref=wo_ref.at[:, theirs], dst_ref=wo_s.at[wide:], send_sem=wo_sem.at[0], recv_sem=wo_sem.at[1],
        device_id=partner, device_id_type=MESH)
    swap_o.start()
    lax.fori_loop(1, blocks, lambda i, _: load_x(i).start(), None)

    def swap_seen(i):
        return pltpu.make_async_remote_copy(
            src_ref=seen_s.at[at(i, BQ), :wide], dst_ref=seen_s.at[at(i, BQ), wide:], send_sem=seen_send.at[i], recv_sem=seen_recv.at[i],
            device_id=partner, device_id_type=MESH)

    def swap_sum(n):
        return pltpu.make_async_remote_copy(
            src_ref=sum_s.at[at(n, PART)], dst_ref=got_s.at[at(n, PART)], send_sem=sum_send.at[n], recv_sem=sum_recv.at[n],
            device_id=peer, device_id_type=MESH)

    def swap_y(n):
        return pltpu.make_async_remote_copy(
            src_ref=y_ref.at[at(n, PART), mine], dst_ref=y_ref.at[at(n, PART), mine], send_sem=y_send.at[n], recv_sem=y_recv.at[n],
            device_id=partner, device_id_type=MESH)

    def come_y(n):
        return pltpu.make_async_remote_copy(
            src_ref=y_ref.at[at(n, PART), theirs], dst_ref=y_ref.at[at(n, PART), theirs], send_sem=y_send.at[n], recv_sem=y_recv.at[n],
            device_id=partner, device_id_type=MESH)

    for n in range(blocks):
        vt_s[n, :, HEAD:, :] = jnp.ones((kv, EXTRA, BQ), BF16)

    def project(i):
        here = at(i, BQ)
        load_x(i).wait()
        for n in range(BQ // 32):
            part = pl.ds(pl.multiple_of(i * BQ + n * 32, 32), 32)
            w = x_s[part, :].astype(F32)
            scale = lax.rsqrt(jnp.sum(w * w, -1, keepdims=True) * (1 / d) + 1e-6)
            a_s[n * 32 : (n + 1) * 32, :] = (w * scale * gain_ref[...].astype(F32)).astype(BF16)

        @pl.when(i == 0)
        def _():
            load_tab.wait()
            load_k.wait()

        low = lax.broadcasted_iota(jnp.int32, (BQ, HEAD), 1) < HEAD // 2
        tab = tab_s[here, :]
        swapped = pltpu.roll(tab, HEAD // 2, 1)
        cos, sin = jnp.where(low, tab, swapped), jnp.where(low, -swapped, tab)

        def turned(t):
            t = t.astype(BF16).astype(F32)
            return (t * cos + pltpu.roll(t, HEAD // 2, 1) * sin).astype(BF16)

        two = 2 * HEAD
        for n in range(kv // 2):
            t = _dot(a_s[...], wk_s[:, n * two : (n + 1) * two], 1, 0)
            for m in range(2):
                k_s[2 * n + m, here, :] = turned(t[:, m * HEAD : (m + 1) * HEAD])
        pl.when(i == 0)(load_v.wait)
        for n in range(kv // 2):
            t = _dot(a_s[...], wv_s[:, n * two : (n + 1) * two], 1, 0)
            for m in range(2):
                vt_s[i, 2 * n + m, :HEAD, :] = t[:, m * HEAD : (m + 1) * HEAD].T.astype(BF16)
        pl.when(i == 0)(load_q.wait)
        for n in range(kv):
            t = _dot(a_s[...], wq_s[:, n * two : (n + 1) * two], 1, 0)
            for m in range(2):
                q_s[n, m * BQ : (m + 1) * BQ, :] = turned(t[:, m * HEAD : (m + 1) * HEAD])

    def attend(i):
        cols = 2 * BQ

        def scores(j):
            return [_dot(k_s[n, at(j, BQ), :], q_s[n], 1, 1) for n in range(kv)]

        ok = lax.rem(lax.broadcasted_iota(jnp.int32, (BQ, cols), 1), BQ) >= lax.broadcasted_iota(jnp.int32, (BQ, cols), 0)
        weights = []
        for n, s in enumerate(scores(i)):
            s = jnp.where(ok, s, HIDDEN)
            top = s.max(axis=0, keepdims=True)
            top_s[n : n + 1, :] = top
            weights.append(jnp.exp2((s - top) * e).astype(BF16))
        for n, p in enumerate(weights):
            mix_s[n] = _dot(vt_s[i, n], p, 1, 0)

        def whole(j, _):
            weights, keeps = [], []
            for n, s in enumerate(scores(j)):
                old = top_s[n : n + 1, :]
                top = jnp.maximum(old, s.max(axis=0, keepdims=True))
                top_s[n : n + 1, :] = top
                weights.append(jnp.exp2((s - top) * e).astype(BF16))
                keeps.append(jnp.exp2((old - top) * e))
            for n, (p, keep) in enumerate(zip(weights, keeps)):
                mix_s[n] = mix_s[n] * keep + _dot(vt_s[j, n], p, 1, 0)

        lax.fori_loop(0, i, whole, None)
        for n in range(kv):
            t = (mix_s[n, :HEAD, :] * (1 / mix_s[n, HEAD : HEAD + 1, :])).T.astype(BF16)
            for m in range(2):
                seen_s[at(i, BQ), (2 * n + m) * HEAD : (2 * n + m + 1) * HEAD] = t[m * BQ : (m + 1) * BQ, :]
        swap_seen(i).start()

    def give(i):
        swap_seen(i).wait_recv()
        for n in range(half // 256):
            t = _dot(seen_s[at(i, BQ), :], wo_s[:, n * 256 : (n + 1) * 256], 1, 0)
            sum_s[at(i, BQ), n * 256 : (n + 1) * 256] = t.astype(BF16)
        for n in range(BQ // PART):
            swap_sum(i * (BQ // PART) + n).start()

    def step(i, _):
        project(i)

        @pl.when(i == 1)
        def _():
            load_o.wait()
            swap_o.wait()

        pl.when(i > 0)(lambda: give(i - 1))
        attend(i)

    lax.fori_loop(0, blocks, step, None)
    give(blocks - 1)

    def finish(n, _):
        here = at(n, PART)
        swap_sum(n).wait_recv()
        both = sum_s[here, :].astype(F32) + got_s[here, :].astype(F32)
        y_ref[here, mine] = (x_s[here, mine].astype(F32) + both).astype(BF16)
        swap_y(n).start()

    lax.fori_loop(0, parts, finish, None)

    def drain(n, _):
        swap_sum(n).wait_send()
        swap_y(n).wait_send()
        come_y(n).wait_recv()

    lax.fori_loop(0, parts, drain, None)
    lax.fori_loop(0, blocks, lambda i, _: swap_seen(i).wait_send(), None)


def solution(mesh):
    def step(x, gain, wq, wk, wv, wo):
        rows, d = x.shape
        heads, kv = wq.shape[1] // HEAD, wk.shape[1] // HEAD
        half = d // 2
        blocks, parts = rows // BQ, rows // PART
        hbm, vmem = pl.BlockSpec(memory_space=pl.ANY), pl.BlockSpec(memory_space=pltpu.VMEM)
        dma = lambda *n: pltpu.SemaphoreType.DMA(n)
        products = 2 * rows * d * (wq.shape[1] + 2 * wk.shape[1]) + 2 * rows * 2 * wo.shape[0] * half
        return pl.pallas_call(
            _kernel,
            out_shape=jax.ShapeDtypeStruct((rows, d), BF16),
            in_specs=[vmem] + [hbm] * 6,
            out_specs=vmem,
            scratch_shapes=[
                pltpu.VMEM((rows, d), BF16),
                pltpu.VMEM(wq.shape, BF16),
                pltpu.VMEM(wk.shape, BF16),
                pltpu.VMEM(wv.shape, BF16),
                pltpu.VMEM((2 * wo.shape[0], half), BF16),
                pltpu.VMEM((rows, HEAD), F32),
                pltpu.VMEM((BQ, d), BF16),
                pltpu.VMEM((kv, 2 * BQ, HEAD), BF16),
                pltpu.VMEM((kv, rows, HEAD), BF16),
                pltpu.VMEM((blocks, kv, HEAD + EXTRA, BQ), BF16),
                pltpu.VMEM((8, 2 * BQ), F32),
                pltpu.VMEM((kv, HEAD + EXTRA, 2 * BQ), F32),
                pltpu.VMEM((rows, 2 * heads * HEAD), BF16),
                pltpu.VMEM((rows, half), BF16),
                pltpu.VMEM((rows, half), BF16),
                dma(5), dma(blocks), dma(2), dma(blocks), dma(blocks), dma(parts), dma(parts), dma(parts), dma(parts),
            ],
            compiler_params=pltpu.CompilerParams(collective_id=0, has_side_effects=True, vmem_limit_bytes=67043328),
            cost_estimate=pl.CostEstimate(flops=products + 2 * rows * rows * heads * HEAD, bytes_accessed=40 * 2**20,
                                          transcendentals=rows * rows * heads // 2),
        )(gain.reshape(1, d), x, wq, wk, wv, wo, jnp.asarray(_rope_table(rows)))

    tokens, columns = P("dp", None), P(None, "tp")
    return jax.shard_map(
        step,
        mesh=mesh,
        in_specs=(tokens, P(None), columns, columns, columns, P("tp", None)),
        out_specs=tokens,
        check_vma=False,
    )
```

```python
import functools

import jax
import jax.numpy as jnp
import numpy as np
from jax import lax
from jax.experimental import pallas as pl
from jax.experimental.pallas import tpu as pltpu
from jax.sharding import PartitionSpec as P

HEAD = 128
THETA = 10000
LOG2E = 1.4426950408889634
HIDDEN = -2e30
BQ = 256
PART = 128
SPAN = 512
EXTRA = 16
F32, BF16 = jnp.float32, jnp.bfloat16
MESH = pl.DeviceIdType.MESH


def _dot(a, b, ca, cb):
    return lax.dot_general(a, b, (((ca,), (cb,)), ((), ())), preferred_element_type=F32)


def _rope_table(rows):
    half = HEAD // 2
    power = np.float32(THETA) ** (-np.arange(half, dtype=np.float32) / np.float32(half))
    angle = np.arange(rows, dtype=np.float32)[:, None] * power.astype(np.float32)
    return np.concatenate([np.cos(angle), np.sin(angle)], -1).astype(np.float32)


def _kernel(gain_ref, x_ref, wq_ref, wk_ref, wv_ref, wo_ref, tab_ref, y_ref,
            x_s, wq_s, wk_s, wv_s, wo_s, tab_s, a_s, q_s, k_s, vt_s, top_s, mix_s, seen_s, sum_s, got_s,
            in_sem, x_sem, wo_sem, seen_send, seen_recv, sum_send, sum_recv, y_send, y_recv):
    rows, d = x_s.shape
    kv = k_s.shape[0]
    wide = seen_s.shape[1] // 2
    chunks, _, span = sum_s.shape
    half = chunks * span
    blocks, messages = rows // BQ, rows // PART * chunks
    e = HEAD**-0.5 * LOG2E
    two = 2 * HEAD
    tp = lax.axis_index("tp")
    core = lax.rem(tp, 2)
    partner = {"tp": tp + 1 - 2 * core}
    peer = {"tp": lax.rem(tp + 2, 4)}
    mine = pl.ds(pl.multiple_of(core * half, half), half)
    theirs = pl.ds(pl.multiple_of((1 - core) * half, half), half)

    def at(i, n, unit=None):
        return pl.ds(pl.multiple_of(i * n, n) if unit is None else pl.multiple_of(i, unit), n)

    barrier = pltpu.get_barrier_semaphore()
    for other in (partner, peer):
        pl.semaphore_signal(barrier, inc=1, device_id=other, device_id_type=MESH)

    def load_x(n):
        return pltpu.make_async_copy(x_ref.at[at(n, PART)], x_s.at[at(n, PART)], x_sem.at[n])

    load_k = pltpu.make_async_copy(wk_ref, wk_s, in_sem.at[0])
    load_v = pltpu.make_async_copy(wv_ref, wv_s, in_sem.at[1])
    load_q = pltpu.make_async_copy(wq_ref, wq_s, in_sem.at[2])
    load_tab = pltpu.make_async_copy(tab_ref.at[:BQ], tab_s.at[:BQ], in_sem.at[3])
    load_rest = pltpu.make_async_copy(tab_ref.at[BQ:], tab_s.at[BQ:], in_sem.at[4])
    load_o = pltpu.make_async_copy(wo_ref.at[:, mine], wo_s.at[:wide], in_sem.at[5])
    swap_o = pltpu.make_async_remote_copy(
        src_ref=wo_ref.at[:, theirs], dst_ref=wo_s.at[wide:], send_sem=wo_sem.at[0], recv_sem=wo_sem.at[1],
        device_id=partner, device_id_type=MESH)

    def swap_seen(m, start, n):
        here = at(start, n, PART)
        return pltpu.make_async_remote_copy(
            src_ref=seen_s.at[here, :wide], dst_ref=seen_s.at[here, wide:], send_sem=seen_send.at[m], recv_sem=seen_recv.at[m],
            device_id=partner, device_id_type=MESH)

    def swap_sum(m):
        chunk, here = lax.rem(m, chunks), at(lax.div(m, chunks), PART)
        return pltpu.make_async_remote_copy(
            src_ref=sum_s.at[chunk, here], dst_ref=got_s.at[chunk, here], send_sem=sum_send.at[m], recv_sem=sum_recv.at[m],
            device_id=peer, device_id_type=MESH)

    def place(m, of):
        return at(lax.div(m, chunks), PART), at(of * chunks + lax.rem(m, chunks), span)

    def swap_y(m, of=core):
        here, cols = place(m, of)
        return pltpu.make_async_remote_copy(
            src_ref=y_ref.at[here, cols], dst_ref=y_ref.at[here, cols], send_sem=y_send.at[m], recv_sem=y_recv.at[m],
            device_id=partner, device_id_type=MESH)

    def norm(start, n):
        gain = gain_ref[...].astype(F32).reshape(1, d)
        for m in range(n // 32):
            w = x_s[pl.ds(pl.multiple_of(start + m * 32, 32), 32), :].astype(F32)
            scale = lax.rsqrt(jnp.sum(w * w, -1, keepdims=True) * (1 / d) + 1e-6)
            a_s[m * 32 : (m + 1) * 32, :] = (w * scale * gain).astype(BF16)

    def turn(start, n):
        low = lax.broadcasted_iota(jnp.int32, (n, HEAD), 1) < HEAD // 2
        tab = tab_s[at(start, n, PART), :]
        swapped = pltpu.roll(tab, HEAD // 2, 1)
        cos, sin = jnp.where(low, tab, swapped), jnp.where(low, -swapped, tab)

        def turned(t):
            t = t.astype(BF16).astype(F32)
            return (t * cos + pltpu.roll(t, HEAD // 2, 1) * sin).astype(BF16)

        return turned

    def keys(start, n):
        turned = turn(start, n)
        for h in range(kv // 2):
            t = _dot(a_s[:n, :], wk_s[:, h * two : (h + 1) * two], 1, 0)
            for m in range(2):
                k_s[2 * h + m, at(start, n, PART), :] = turned(t[:, m * HEAD : (m + 1) * HEAD])

    def values(i, off, n):
        for h in range(kv // 2):
            t = _dot(a_s[:n, :], wv_s[:, h * two : (h + 1) * two], 1, 0)
            for m in range(2):
                vt_s[i, 2 * h + m, :HEAD, off : off + n] = t[:, m * HEAD : (m + 1) * HEAD].T.astype(BF16)

    def queries(start, n):
        turned = turn(start, n)
        for h in range(kv):
            t = _dot(a_s[:n, :], wq_s[:, h * two : (h + 1) * two], 1, 0)
            for m in range(2):
                q_s[h, m * n : (m + 1) * n, :] = turned(t[:, m * HEAD : (m + 1) * HEAD])

    def attend(i, off, n):
        cols, ends = 2 * n, off + n

        def scores(h, start, size):
            return _dot(k_s[h, at(start, size, PART), :], q_s[h, :cols, :], 1, 1)

        gap = lax.rem(lax.broadcasted_iota(jnp.int32, (ends, cols), 1), n) - lax.broadcasted_iota(jnp.int32, (ends, cols), 0)
        weights = []
        for h, s in enumerate([scores(h, i * BQ, ends) for h in range(kv)]):
            s = jnp.where(gap >= -off, s, HIDDEN)
            top = s.max(axis=0, keepdims=True)
            top_s[h : h + 1, :cols] = top
            weights.append(jnp.exp2((s - top) * e).astype(BF16))
        for h, p in enumerate(weights):
            mix_s[h, :, :cols] = _dot(vt_s[i, h, :, :ends], p, 1, 0)

        def whole(j, _):
            weights, keeps = [], []
            for h, s in enumerate([scores(h, j * BQ, BQ) for h in range(kv)]):
                old = top_s[h : h + 1, :cols]
                top = jnp.maximum(old, s.max(axis=0, keepdims=True))
                top_s[h : h + 1, :cols] = top
                weights.append(jnp.exp2((s - top) * e).astype(BF16))
                keeps.append(jnp.exp2((old - top) * e))
            for h, (p, keep) in enumerate(zip(weights, keeps)):
                mix_s[h, :, :cols] = mix_s[h, :, :cols] * keep + _dot(vt_s[j, h], p, 1, 0)

        if not isinstance(i, int):
            lax.fori_loop(0, i, whole, None)
        for h in range(kv):
            t = (mix_s[h, :HEAD, :cols] * (1 / mix_s[h, HEAD : HEAD + 1, :cols])).T.astype(BF16)
            for m in range(2):
                seen_s[at(i * BQ + off, n, PART), (2 * h + m) * HEAD : (2 * h + m + 1) * HEAD] = t[m * n : (m + 1) * n, :]

    def give(start, n):
        here = at(start, n, PART)
        for chunk in range(chunks):
            for m in range(span // two):
                left = chunk * span + m * two
                sum_s[chunk, here, m * two : (m + 1) * two] = _dot(seen_s[here, :], wo_s[:, left : left + two], 1, 0).astype(BF16)
            for m in range(n // PART):
                swap_sum((lax.div(start, PART) + m) * chunks + chunk).start()

    load_x(0).start()
    load_tab.start()
    load_k.start()
    load_v.start()
    for n in range(blocks):
        vt_s[n, :, HEAD:, :] = jnp.ones((kv, EXTRA, BQ), BF16)
    load_x(0).wait()
    load_q.start()
    norm(0, PART)
    load_tab.wait()
    load_k.wait()
    load_o.start()
    load_x(1).start()
    keys(0, PART)
    load_v.wait()
    values(0, 0, PART)
    pl.semaphore_wait(barrier, 2)
    swap_o.start()
    load_q.wait()
    load_rest.start()
    lax.fori_loop(2, 2 * blocks, lambda n, _: load_x(n).start(), None)
    queries(0, PART)
    attend(0, 0, PART)
    swap_seen(0, 0, PART).start()
    load_x(1).wait()
    norm(PART, PART)
    keys(PART, PART)
    load_o.wait()
    swap_o.wait()
    swap_seen(0, 0, PART).wait_recv()
    give(0, PART)
    values(0, PART, PART)
    queries(PART, PART)
    attend(0, PART, PART)
    swap_seen(1, PART, PART).start()
    load_rest.wait()

    def step(i, _):
        start = i * BQ
        for m in range(BQ // PART):
            load_x(i * (BQ // PART) + m).wait()
        norm(start, BQ)
        keys(start, BQ)
        values(i, 0, BQ)

        @pl.when(i == 1)
        def _():
            swap_seen(1, PART, PART).wait_recv()
            give(PART, PART)

        @pl.when(i > 1)
        def _():
            swap_seen(i, start - BQ, BQ).wait_recv()
            give(start - BQ, BQ)

        queries(start, BQ)
        attend(i, 0, BQ)
        swap_seen(i + 1, start, BQ).start()

    lax.fori_loop(1, blocks, step, None)
    swap_seen(blocks, rows - BQ, BQ).wait_recv()
    give(rows - BQ, BQ)

    def finish(m, _):
        swap_sum(m).wait_recv()
        chunk, (here, cols) = lax.rem(m, chunks), place(m, core)
        both = sum_s[chunk, here, :].astype(F32) + got_s[chunk, here, :].astype(F32)
        y_ref[here, cols] = (x_s[here, cols].astype(F32) + both).astype(BF16)
        swap_y(m).start()

    lax.fori_loop(0, messages, finish, None)

    def drain(m, _):
        swap_sum(m).wait_send()
        swap_y(m).wait_send()
        swap_y(m, 1 - core).wait_recv()

    lax.fori_loop(0, messages, drain, None)
    for m in range(2):
        swap_seen(m, m * PART, PART).wait_send()
    lax.fori_loop(1, blocks, lambda i, _: swap_seen(i + 1, i * BQ, BQ).wait_send(), None)


def solution(mesh):
    def step(x, gain, wq, wk, wv, wo):
        rows, d = x.shape
        heads, kv = wq.shape[1] // HEAD, wk.shape[1] // HEAD
        half = d // 2
        blocks, parts, messages = rows // BQ, rows // PART, rows // PART * (half // SPAN)
        hbm, vmem = pl.BlockSpec(memory_space=pl.ANY), pl.BlockSpec(memory_space=pltpu.VMEM)
        dma = lambda *n: pltpu.SemaphoreType.DMA(n)
        products = 2 * rows * d * (wq.shape[1] + 2 * wk.shape[1]) + 2 * rows * 2 * wo.shape[0] * half
        return pl.pallas_call(
            _kernel,
            out_shape=pltpu.VMEM((rows, d), BF16),
            in_specs=[vmem] + [hbm] * 6,
            out_specs=vmem,
            scratch_shapes=[
                pltpu.VMEM((rows, d), BF16),
                pltpu.VMEM(wq.shape, BF16),
                pltpu.VMEM(wk.shape, BF16),
                pltpu.VMEM(wv.shape, BF16),
                pltpu.VMEM((2 * wo.shape[0], half), BF16),
                pltpu.VMEM((rows, HEAD), F32),
                pltpu.VMEM((BQ, d), BF16),
                pltpu.VMEM((kv, 2 * BQ, HEAD), BF16),
                pltpu.VMEM((kv, rows, HEAD), BF16),
                pltpu.VMEM((blocks, kv, HEAD + EXTRA, BQ), BF16),
                pltpu.VMEM((8, 2 * BQ), F32),
                pltpu.VMEM((kv, HEAD + EXTRA, 2 * BQ), F32),
                pltpu.VMEM((rows, 2 * heads * HEAD), BF16),
                pltpu.VMEM((half // SPAN, rows, SPAN), BF16),
                pltpu.VMEM((half // SPAN, rows, SPAN), BF16),
                dma(6), dma(parts), dma(2), dma(blocks + 1), dma(blocks + 1), dma(messages), dma(messages), dma(messages), dma(messages),
            ],
            compiler_params=pltpu.CompilerParams(collective_id=0, has_side_effects=True, vmem_limit_bytes=54 * 2**20),
            cost_estimate=pl.CostEstimate(flops=products + 2 * rows * rows * heads * HEAD, bytes_accessed=40 * 2**20,
                                          transcendentals=rows * rows * heads // 2),
        )(gain, x, wq, wk, wv, wo, jnp.asarray(_rope_table(rows)))

    tokens, columns = P("dp", None), P(None, "tp")
    return jax.shard_map(
        step,
        mesh=mesh,
        in_specs=(tokens, P(None), columns, columns, columns, P("tp", None)),
        out_specs=tokens,
        check_vma=False,
    )
```

```python
import functools

import jax
import jax.numpy as jnp
import numpy as np
from jax import lax
from jax.experimental import pallas as pl
from jax.experimental.pallas import tpu as pltpu
from jax.sharding import PartitionSpec as P

HEAD = 128
THETA = 10000
LOG2E = 1.4426950408889634
HIDDEN = -2e30
BQ = 256
PART = 128
EARLY = 512
SPAN = 512
TAIL = 64
EXTRA = 16
F32, BF16 = jnp.float32, jnp.bfloat16
MESH = pl.DeviceIdType.MESH


def _dot(a, b, ca, cb):
    return lax.dot_general(a, b, (((ca,), (cb,)), ((), ())), preferred_element_type=F32)


def _rope_table(rows):
    half = HEAD // 2
    power = np.float32(THETA) ** (-np.arange(half, dtype=np.float32) / np.float32(half))
    angle = np.arange(rows, dtype=np.float32)[:, None] * power.astype(np.float32)
    return np.concatenate([np.cos(angle), np.sin(angle)], -1).astype(np.float32)


def _kernel(gain_ref, x_ref, wq_ref, wk_ref, wv_ref, wo_ref, tab_ref, y_ref,
            x_s, wq_s, wk_s, wv_s, wo_s, tab_s, a_s, q_s, k_s, vt_s, top_s, mix_s, seen_s, sum_s, got_s,
            in_sem, wo_sem, seen_recv, sum_recv, all_sem):
    rows, d = x_s.shape
    kv = k_s.shape[0]
    wide = seen_s.shape[1] // 2
    chunks = sum_s.shape[0]
    half = chunks * SPAN
    blocks, last = rows // BQ, rows - BQ
    e = HEAD**-0.5 * LOG2E
    two = 2 * HEAD
    tp = lax.axis_index("tp")
    core = lax.rem(tp, 2)
    partner = {"tp": tp + 1 - 2 * core}
    peer = {"tp": lax.rem(tp + 2, 4)}
    mine = pl.ds(pl.multiple_of(core * half, half), half)
    theirs = pl.ds(pl.multiple_of((1 - core) * half, half), half)

    def at(start, n):
        return pl.ds(pl.multiple_of(start, min(n, PART)), n)

    barrier = pltpu.get_barrier_semaphore()
    for other in (partner, peer):
        pl.semaphore_signal(barrier, inc=1, device_id=other, device_id_type=MESH)

    def load_x(m):
        here = pl.ds((0, PART, EARLY)[m], (PART, EARLY - PART, rows - EARLY)[m])
        return pltpu.make_async_copy(x_ref.at[here], x_s.at[here], in_sem.at[m])

    load_k = pltpu.make_async_copy(wk_ref, wk_s, in_sem.at[3])
    load_v = pltpu.make_async_copy(wv_ref, wv_s, in_sem.at[4])
    load_q = pltpu.make_async_copy(wq_ref, wq_s, in_sem.at[5])
    load_tab = pltpu.make_async_copy(tab_ref.at[:EARLY], tab_s.at[:EARLY], in_sem.at[6])
    load_rest = pltpu.make_async_copy(tab_ref.at[EARLY:], tab_s.at[EARLY:], in_sem.at[7])
    load_o = pltpu.make_async_copy(wo_ref.at[:, mine], wo_s.at[:wide], in_sem.at[8])
    swap_o = pltpu.make_async_remote_copy(
        src_ref=wo_ref.at[:, theirs], dst_ref=wo_s.at[wide:], send_sem=wo_sem.at[0], recv_sem=wo_sem.at[1],
        device_id=partner, device_id_type=MESH)


    def swap_seen(m, start, n):
        here = at(start, n)
        return pltpu.make_async_remote_copy(
            src_ref=seen_s.at[here, :wide], dst_ref=seen_s.at[here, wide:], send_sem=all_sem.at[0], recv_sem=seen_recv.at[m],
            device_id=partner, device_id_type=MESH)

    def swap_sum(m, first, count, start, n):
        here = at(start, n)
        return pltpu.make_async_remote_copy(
            src_ref=sum_s.at[first : first + count, here], dst_ref=got_s.at[first : first + count, here],
            send_sem=all_sem.at[1], recv_sem=sum_recv.at[m], device_id=peer, device_id_type=MESH)

    def swap_y(here, cols):
        return pltpu.make_async_remote_copy(
            src_ref=y_ref.at[here, cols], dst_ref=y_ref.at[here, cols], send_sem=all_sem.at[2], recv_sem=all_sem.at[3],
            device_id=partner, device_id_type=MESH)

    def norm(start, n):
        gain = gain_ref[...].astype(F32).reshape(1, d)
        for m in range(n // 32):
            w = x_s[pl.ds(pl.multiple_of(start + m * 32, 32), 32), :].astype(F32)
            scale = lax.rsqrt(jnp.sum(w * w, -1, keepdims=True) * (1 / d) + 1e-6)
            a_s[m * 32 : (m + 1) * 32, :] = (w * scale * gain).astype(BF16)

    def turn(start, n):
        low = lax.broadcasted_iota(jnp.int32, (n, HEAD), 1) < HEAD // 2
        tab = tab_s[at(start, n), :]
        swapped = pltpu.roll(tab, HEAD // 2, 1)
        cos, sin = jnp.where(low, tab, swapped), jnp.where(low, -swapped, tab)

        def turned(t):
            t = t.astype(BF16).astype(F32)
            return (t * cos + pltpu.roll(t, HEAD // 2, 1) * sin).astype(BF16)

        return turned

    def keys(start, n):
        turned = turn(start, n)
        for h in range(kv // 2):
            t = _dot(a_s[:n, :], wk_s[:, h * two : (h + 1) * two], 1, 0)
            for m in range(2):
                k_s[2 * h + m, at(start, n), :] = turned(t[:, m * HEAD : (m + 1) * HEAD])

    def values(i, off, n):
        for h in range(kv // 2):
            t = _dot(a_s[:n, :], wv_s[:, h * two : (h + 1) * two], 1, 0)
            for m in range(2):
                vt_s[i, 2 * h + m, :HEAD, off : off + n] = t[:, m * HEAD : (m + 1) * HEAD].T.astype(BF16)

    def queries(start, n):
        turned = turn(start, n)
        for h in range(kv):
            t = _dot(a_s[:n, :], wq_s[:, h * two : (h + 1) * two], 1, 0)
            for m in range(2):
                q_s[h, m * n : (m + 1) * n, :] = turned(t[:, m * HEAD : (m + 1) * HEAD])

    def attend(i, off, n):
        cols, ends = 2 * n, off + n

        def scores(h, start, size):
            return _dot(k_s[h, at(start, size), :], q_s[h, :cols, :], 1, 1)

        gap = lax.rem(lax.broadcasted_iota(jnp.int32, (ends, cols), 1), n) - lax.broadcasted_iota(jnp.int32, (ends, cols), 0)
        weights = []
        for h, s in enumerate([scores(h, i * BQ, ends) for h in range(kv)]):
            s = jnp.where(gap >= -off, s, HIDDEN)
            top = s.max(axis=0, keepdims=True)
            top_s[h : h + 1, :cols] = top
            weights.append(jnp.exp2((s - top) * e).astype(BF16))
        for h, p in enumerate(weights):
            mix_s[h, :, :cols] = _dot(vt_s[i, h, :, :ends], p, 1, 0)

        def whole(j, _):
            weights, keeps = [], []
            for h, s in enumerate([scores(h, j * BQ, BQ) for h in range(kv)]):
                old = top_s[h : h + 1, :cols]
                top = jnp.maximum(old, s.max(axis=0, keepdims=True))
                top_s[h : h + 1, :cols] = top
                weights.append(jnp.exp2((s - top) * e).astype(BF16))
                keeps.append(jnp.exp2((old - top) * e))
            for h, (p, keep) in enumerate(zip(weights, keeps)):
                mix_s[h, :, :cols] = mix_s[h, :, :cols] * keep + _dot(vt_s[j, h], p, 1, 0)

        if isinstance(i, int):
            for j in range(i):
                whole(j, None)
        else:
            lax.fori_loop(0, i, whole, None)
        for h in range(kv):
            t = (mix_s[h, :HEAD, :cols] * (1 / mix_s[h, HEAD : HEAD + 1, :cols])).T.astype(BF16)
            for m in range(2):
                seen_s[at(i * BQ + off, n), (2 * h + m) * HEAD : (2 * h + m + 1) * HEAD] = t[m * n : (m + 1) * n, :]

    def give(m, start, n, tail=False):
        here = at(start, n)
        swap_seen(m, start, n).wait_recv()
        for chunk in range(chunks):
            for col in range(0, SPAN, two):
                left = chunk * SPAN + col
                sum_s[chunk, here, col : col + two] = _dot(seen_s[here, :], wo_s[:, left : left + two], 1, 0).astype(BF16)
            if not tail:
                swap_sum(lax.div(start, BQ), chunk, 1, start, n).start()
            elif chunk < chunks - 1:
                swap_sum(blocks - 1 + chunk, chunk, 1, start, n).start()
            else:
                for r in range(n // TAIL):
                    swap_sum(blocks - 1 + chunk + r, chunk, 1, start + r * TAIL, TAIL).start()

    load_x(0).start()
    load_tab.start()
    load_k.start()
    load_q.start()
    load_v.start()
    pl.semaphore_wait(barrier, 2)
    load_x(0).wait()
    norm(0, PART)
    load_tab.wait()
    load_k.wait()
    swap_o.start()
    load_x(1).start()
    load_o.start()
    for n in range(blocks):
        vt_s[n, :, HEAD:, :] = jnp.ones((kv, EXTRA, BQ), BF16)
    keys(0, PART)
    load_q.wait()
    queries(0, PART)
    load_v.wait()
    values(0, 0, PART)
    attend(0, 0, PART)
    swap_seen(0, 0, PART).start()
    load_x(1).wait()
    for m in range(1, EARLY // PART):
        start = m * PART
        norm(start, PART)
        keys(start, PART)
        if m == 1:
            load_o.wait()
            swap_o.wait()
            load_rest.start()
            load_x(2).start()
        give(m - 1, start - PART, PART)
        values(start // BQ, start % BQ, PART)
        queries(start, PART)
        attend(start // BQ, start % BQ, PART)
        swap_seen(m, start, PART).start()
    load_rest.wait()
    load_x(2).wait()
    more = EARLY // PART - EARLY // BQ

    def step(i, _):
        start = i * BQ
        norm(start, BQ)
        keys(start, BQ)
        values(i, 0, BQ)

        @pl.when(i == EARLY // BQ)
        def _():
            give(EARLY // PART - 1, EARLY - PART, PART)

        @pl.when(i > EARLY // BQ)
        def _():
            give(i - 1 + more, start - BQ, BQ)

        queries(start, BQ)
        attend(i, 0, BQ)
        swap_seen(i + more, start, BQ).start()

    lax.fori_loop(EARLY // BQ, blocks, step, None)
    give(blocks - 1 + more, last, BQ, tail=True)

    def finish(start, n, first, count):
        here = at(start, n)
        for chunk in range(first, first + count):
            cols = pl.ds(pl.multiple_of(core * half + chunk * SPAN, SPAN), SPAN)
            both = sum_s[chunk, here, :].astype(F32) + got_s[chunk, here, :].astype(F32)
            y_ref[here, cols] = (x_s[here, cols].astype(F32) + both).astype(BF16)
        swap_y(here, pl.ds(pl.multiple_of(core * half + first * SPAN, SPAN), count * SPAN)).start()

    def finish_block(i, _):
        swap_sum(i, 0, chunks, i * BQ, BQ).wait_recv()
        finish(i * BQ, BQ, 0, chunks)

    lax.fori_loop(0, blocks - 1, finish_block, None)
    for chunk in range(chunks - 1):
        swap_sum(blocks - 1 + chunk, chunk, 1, last, BQ).wait_recv()
        finish(last, BQ, chunk, 1)
    for r in range(BQ // TAIL):
        swap_sum(blocks - 1 + chunks - 1 + r, chunks - 1, 1, last + r * TAIL, TAIL).wait_recv()
        finish(last + r * TAIL, TAIL, chunks - 1, 1)
    swap_seen(0, 0, rows).wait_send()
    swap_sum(0, 0, chunks, 0, rows).wait_send()
    swap_y(pl.ds(0, rows), mine).wait_send()
    swap_y(pl.ds(0, rows), theirs).wait_recv()


def solution(mesh):
    def step(x, gain, wq, wk, wv, wo):
        rows, d = x.shape
        heads, kv = wq.shape[1] // HEAD, wk.shape[1] // HEAD
        half = d // 2
        blocks = rows // BQ
        hbm, vmem = pl.BlockSpec(memory_space=pl.ANY), pl.BlockSpec(memory_space=pltpu.VMEM)
        dma = lambda *n: pltpu.SemaphoreType.DMA(n)
        products = 2 * rows * d * (wq.shape[1] + 2 * wk.shape[1]) + 2 * rows * 2 * wo.shape[0] * half
        return pl.pallas_call(
            _kernel,
            out_shape=pltpu.VMEM((rows, d), BF16),
            in_specs=[vmem] + [hbm] * 6,
            out_specs=vmem,
            scratch_shapes=[
                pltpu.VMEM((rows, d), BF16),
                pltpu.VMEM(wq.shape, BF16),
                pltpu.VMEM(wk.shape, BF16),
                pltpu.VMEM(wv.shape, BF16),
                pltpu.VMEM((2 * wo.shape[0], half), BF16),
                pltpu.VMEM((rows, HEAD), F32),
                pltpu.VMEM((BQ, d), BF16),
                pltpu.VMEM((kv, 2 * BQ, HEAD), BF16),
                pltpu.VMEM((kv, rows, HEAD), BF16),
                pltpu.VMEM((blocks, kv, HEAD + EXTRA, BQ), BF16),
                pltpu.VMEM((8, 2 * BQ), F32),
                pltpu.VMEM((kv, HEAD + EXTRA, 2 * BQ), F32),
                pltpu.VMEM((rows, 2 * heads * HEAD), BF16),
                pltpu.VMEM((half // SPAN, rows, SPAN), BF16),
                pltpu.VMEM((half // SPAN, rows, SPAN), BF16),
                dma(9), dma(2), dma(EARLY // PART + blocks - EARLY // BQ), dma(blocks - 1 + half // SPAN - 1 + BQ // TAIL), dma(4),
            ],
            compiler_params=pltpu.CompilerParams(collective_id=0, has_side_effects=True, vmem_limit_bytes=54 * 2**20),
            cost_estimate=pl.CostEstimate(flops=products + 2 * rows * rows * heads * HEAD, bytes_accessed=40 * 2**20,
                                          transcendentals=rows * rows * heads // 2),
        )(gain, x, wq, wk, wv, wo, jnp.asarray(_rope_table(rows)))

    tokens, columns = P("dp", None), P(None, "tp")
    return jax.shard_map(
        step,
        mesh=mesh,
        in_specs=(tokens, P(None), columns, columns, columns, P("tp", None)),
        out_specs=tokens,
        check_vma=False,
    )
```

```python
import functools

import jax
import jax.numpy as jnp
import numpy as np
from jax import lax
from jax.experimental import pallas as pl
from jax.experimental.pallas import tpu as pltpu
from jax.sharding import PartitionSpec as P

HEAD = 128
THETA = 10000
LOG2E = 1.4426950408889634
HIDDEN = -2e30
BQ = 256
PART = 128
SPAN = 512
TAIL = ((0, 64), (64, 32), (96, 32))
EXTRA = 16
F32, BF16 = jnp.float32, jnp.bfloat16
MESH = pl.DeviceIdType.MESH


def _dot(a, b, ca, cb):
    return lax.dot_general(a, b, (((ca,), (cb,)), ((), ())), preferred_element_type=F32)


def _rope_table(rows):
    half = HEAD // 2
    power = np.float32(THETA) ** (-np.arange(half, dtype=np.float32) / np.float32(half))
    angle = np.arange(rows, dtype=np.float32)[:, None] * power.astype(np.float32)
    return np.concatenate([np.cos(angle), np.sin(angle)], -1).astype(np.float32)


def _kernel(gain_ref, x_ref, wq_ref, wk_ref, wv_ref, wo_ref, tab_ref, y_ref,
            x_s, gain_s, wq_s, wk_s, wv_s, wo_s, tab_s, a_s, q_s, k_s, vt_s, top_s, mix_s, seen_s, sum_s, got_s,
            in_sem, wo_sem, seen_recv, sum_recv, all_sem):
    rows, d = x_s.shape
    kv = k_s.shape[0]
    wide = seen_s.shape[1] // 2
    chunks = sum_s.shape[0]
    half = chunks * SPAN
    blocks, subs, last = rows // BQ, rows // PART, rows - BQ
    e = HEAD**-0.5 * LOG2E
    two = 2 * HEAD
    tp = lax.axis_index("tp")
    core = lax.rem(tp, 2)
    partner = {"tp": tp + 1 - 2 * core}
    peer = {"tp": lax.rem(tp + 2, 4)}
    mine = pl.ds(pl.multiple_of(core * half, half), half)
    theirs = pl.ds(pl.multiple_of((1 - core) * half, half), half)

    def at(start, n):
        return pl.ds(pl.multiple_of(start, min(n, PART)), n)

    barrier = pltpu.get_barrier_semaphore()
    for other in (partner, peer):
        pl.semaphore_signal(barrier, inc=1, device_id=other, device_id_type=MESH)

    def load_x(m):
        edges = (0, PART, BQ, 2 * BQ, rows)
        here = pl.ds(edges[m], edges[m + 1] - edges[m])
        return pltpu.make_async_copy(x_ref.at[here], x_s.at[here], in_sem.at[m])

    def load_q(m):
        cols = pl.ds(m * wide // 2, wide // 2)
        return pltpu.make_async_copy(wq_ref.at[:, cols], wq_s.at[:, cols], in_sem.at[4 + m])

    load_k = pltpu.make_async_copy(wk_ref, wk_s, in_sem.at[6])
    load_v = pltpu.make_async_copy(wv_ref, wv_s, in_sem.at[7])
    load_gain = pltpu.make_async_copy(gain_ref, gain_s, in_sem.at[8])
    load_tab = pltpu.make_async_copy(tab_ref.at[:BQ], tab_s.at[:BQ], in_sem.at[9])
    load_rest = pltpu.make_async_copy(tab_ref.at[BQ:], tab_s.at[BQ:], in_sem.at[10])
    load_o = pltpu.make_async_copy(wo_ref.at[:, mine], wo_s.at[:wide], in_sem.at[11])

    def swap_o(m):
        cols = pl.ds(pl.multiple_of((1 - core) * half + m * SPAN, SPAN), SPAN)
        return pltpu.make_async_remote_copy(
            src_ref=wo_ref.at[:, cols], dst_ref=wo_s.at[wide:, m * SPAN : (m + 1) * SPAN],
            send_sem=wo_sem.at[chunks], recv_sem=wo_sem.at[m], device_id=partner, device_id_type=MESH)

    sent_o = pltpu.make_async_remote_copy(
        src_ref=wo_ref.at[:, theirs], dst_ref=wo_s.at[wide:], send_sem=wo_sem.at[chunks], recv_sem=wo_sem.at[0],
        device_id=partner, device_id_type=MESH)


    def swap_seen(m, n=PART):
        here = at(m * PART, n)
        return pltpu.make_async_remote_copy(
            src_ref=seen_s.at[here, :wide], dst_ref=seen_s.at[here, wide:], send_sem=all_sem.at[0], recv_sem=seen_recv.at[m],
            device_id=partner, device_id_type=MESH)

    def swap_sum(m, first, count, start, n):
        here = at(start, n)
        return pltpu.make_async_remote_copy(
            src_ref=sum_s.at[first : first + count, here], dst_ref=got_s.at[first : first + count, here],
            send_sem=all_sem.at[1], recv_sem=sum_recv.at[m], device_id=peer, device_id_type=MESH)

    def swap_y(here, cols):
        return pltpu.make_async_remote_copy(
            src_ref=y_ref.at[here, cols], dst_ref=y_ref.at[here, cols], send_sem=all_sem.at[2], recv_sem=all_sem.at[3],
            device_id=partner, device_id_type=MESH)

    def norm(start, n):
        gain = gain_s[...].astype(F32).reshape(1, d)
        for m in range(n // 32):
            w = x_s[pl.ds(pl.multiple_of(start + m * 32, 32), 32), :].astype(F32)
            scale = lax.rsqrt(jnp.sum(w * w, -1, keepdims=True) * (1 / d) + 1e-6)
            a_s[m * 32 : (m + 1) * 32, :] = (w * scale * gain).astype(BF16)

    def turn(start, n):
        low = lax.broadcasted_iota(jnp.int32, (n, HEAD), 1) < HEAD // 2
        tab = tab_s[at(start, n), :]
        swapped = pltpu.roll(tab, HEAD // 2, 1)
        cos, sin = jnp.where(low, tab, swapped), jnp.where(low, -swapped, tab)

        def turned(t):
            t = t.astype(BF16).astype(F32)
            return (t * cos + pltpu.roll(t, HEAD // 2, 1) * sin).astype(BF16)

        return turned

    def keys(start, n):
        turned = turn(start, n)
        for h in range(kv // 2):
            t = _dot(a_s[:n, :], wk_s[:, h * two : (h + 1) * two], 1, 0)
            for m in range(2):
                k_s[2 * h + m, at(start, n), :] = turned(t[:, m * HEAD : (m + 1) * HEAD])

    def values(i, off, n):
        for h in range(kv // 2):
            t = _dot(a_s[:n, :], wv_s[:, h * two : (h + 1) * two], 1, 0)
            for m in range(2):
                vt_s[i, 2 * h + m, :HEAD, off : off + n] = t[:, m * HEAD : (m + 1) * HEAD].T.astype(BF16)

    def queries(start, n, heads=None):
        turned = turn(start, n)
        for h in range(kv) if heads is None else heads:
            t = _dot(a_s[:n, :], wq_s[:, h * two : (h + 1) * two], 1, 0)
            for m in range(2):
                q_s[h, m * n : (m + 1) * n, :] = turned(t[:, m * HEAD : (m + 1) * HEAD])

    def attend(i, off, row, stride):
        n, cols, ends = PART, 2 * PART, off + PART

        def scores(h, start, size):
            q = jnp.concatenate([q_s[h, m * stride + row : m * stride + row + n, :] for m in range(2)], axis=0)
            return _dot(k_s[h, at(start, size), :], q, 1, 1)

        gap = lax.rem(lax.broadcasted_iota(jnp.int32, (ends, cols), 1), n) - lax.broadcasted_iota(jnp.int32, (ends, cols), 0)
        weights = []
        for h, s in enumerate([scores(h, i * BQ, ends) for h in range(kv)]):
            s = jnp.where(gap >= -off, s, HIDDEN)
            top = s.max(axis=0, keepdims=True)
            top_s[h : h + 1, :cols] = top
            weights.append(jnp.exp2((s - top) * e).astype(BF16))
        for h, p in enumerate(weights):
            mix_s[h, :, :cols] = _dot(vt_s[i, h, :, :ends], p, 1, 0)

        def whole(j, many):
            weights, keeps = [], []
            for h, s in enumerate([scores(h, j * BQ, many * BQ) for h in range(kv)]):
                old = top_s[h : h + 1, :cols]
                top = jnp.maximum(old, s.max(axis=0, keepdims=True))
                top_s[h : h + 1, :cols] = top
                weights.append(jnp.exp2((s - top) * e).astype(BF16))
                keeps.append(jnp.exp2((old - top) * e))
            for h, (p, keep) in enumerate(zip(weights, keeps)):
                mix = mix_s[h, :, :cols] * keep
                for m in range(many):
                    mix = mix + _dot(vt_s[j + m, h], p[m * BQ : (m + 1) * BQ], 1, 0)
                mix_s[h, :, :cols] = mix

        if not isinstance(i, int):
            lax.fori_loop(0, lax.div(i, 2), lambda j, _: whole(2 * j, 2), None)
            pl.when(lax.rem(i, 2) == 1)(lambda: whole(i - 1, 1))
        for h in range(kv):
            t = (mix_s[h, :HEAD, :cols] * (1 / mix_s[h, HEAD : HEAD + 1, :cols])).T.astype(BF16)
            for m in range(2):
                seen_s[at(i * BQ + off, n), (2 * h + m) * HEAD : (2 * h + m + 1) * HEAD] = t[m * n : (m + 1) * n, :]

    def send(m, chunk):
        if not isinstance(m, int):
            swap_sum(lax.div(m, BQ // PART), chunk, 1, m * PART, PART).start()
        elif m < subs - 2:
            swap_sum(m // (BQ // PART), chunk, 1, m * PART, PART).start()
        elif m == subs - 2:
            swap_sum(blocks - 1, chunk, 1, m * PART, PART).start()
        elif chunk < chunks - 1:
            swap_sum(blocks + chunk, chunk, 1, m * PART, PART).start()
        else:
            for r, (row, size) in enumerate(TAIL):
                swap_sum(blocks + chunks - 1 + r, chunk, 1, m * PART + row, size).start()

    def give(m):
        here = at(m * PART, PART)
        swap_seen(m).wait_recv()
        for chunk in range(chunks):
            for col in range(0, SPAN, two):
                left = chunk * SPAN + col
                sum_s[chunk, here, col : col + two] = _dot(seen_s[here, :], wo_s[:, left : left + two], 1, 0).astype(BF16)
            send(m, chunk)

    def give_first():
        load_o.wait()
        for m in range(half // two):
            mix_s[m, :PART, :two] = _dot(seen_s[:PART, :wide], wo_s[:wide, m * two : (m + 1) * two], 1, 0)
        load_x(1).wait()
        norm(PART, PART)
        for chunk in range(chunks):
            swap_o(chunk).wait_recv()
            if chunk == 0:
                swap_seen(0).wait_recv()
            for col in range(0, SPAN, two):
                m = (chunk * SPAN + col) // two
                t = mix_s[m, :PART, :two] + _dot(seen_s[:PART, wide:], wo_s[wide:, m * two : (m + 1) * two], 1, 0)
                sum_s[chunk, :PART, col : col + two] = t.astype(BF16)
            send(0, chunk)

    load_x(0).start()
    load_gain.start()
    load_tab.start()
    load_k.start()
    load_v.start()
    load_q(0).start()
    load_q(1).start()
    pl.semaphore_wait(barrier, 2)
    for chunk in range(chunks):
        swap_o(chunk).start()
    load_gain.wait()
    load_x(0).wait()
    norm(0, PART)
    load_tab.wait()
    load_k.wait()
    load_o.start()
    load_x(1).start()
    for n in range(blocks):
        vt_s[n, :, HEAD:, :] = jnp.ones((kv, EXTRA, BQ), BF16)
    keys(0, PART)
    load_v.wait()
    values(0, 0, PART)
    load_q(0).wait()
    queries(0, PART, range(kv // 2))
    load_q(1).wait()
    load_x(2).start()
    load_rest.start()
    queries(0, PART, range(kv // 2, kv))
    attend(0, 0, 0, PART)
    swap_seen(0).start()
    load_x(3).start()
    give_first()
    keys(PART, PART)
    values(0, PART, PART)
    queries(PART, PART)
    attend(0, PART, 0, PART)
    swap_seen(1).start()
    load_x(2).wait()
    load_rest.wait()
    norm(BQ, BQ)
    keys(BQ, BQ)
    give(1)
    load_x(3).wait()

    def step(i, _):
        start = i * BQ
        values(i, 0, BQ)
        queries(start, BQ)
        pl.when(i > 1)(lambda: give(2 * i - 1))
        attend(i, 0, 0, BQ)
        swap_seen(2 * i).start()

        @pl.when(i < blocks - 1)
        def _():
            norm(start + BQ, BQ)
            keys(start + BQ, BQ)
            give(2 * i)

        pl.when(i == blocks - 1)(lambda: give(subs - 2))
        attend(i, PART, PART, BQ)
        swap_seen(2 * i + 1).start()

    lax.fori_loop(1, blocks, step, None)
    give(subs - 1)

    def finish(start, n, first, count):
        here = at(start, n)
        for chunk in range(first, first + count):
            cols = pl.ds(pl.multiple_of(core * half + chunk * SPAN, SPAN), SPAN)
            both = sum_s[chunk, here, :].astype(F32) + got_s[chunk, here, :].astype(F32)
            y_ref[here, cols] = (x_s[here, cols].astype(F32) + both).astype(BF16)
        swap_y(here, pl.ds(pl.multiple_of(core * half + first * SPAN, SPAN), count * SPAN)).start()

    def finish_block(i, _):
        swap_sum(i, 0, chunks, i * BQ, BQ).wait_recv()
        finish(i * BQ, BQ, 0, chunks)

    lax.fori_loop(0, blocks - 1, finish_block, None)
    swap_sum(blocks - 1, 0, chunks, last, PART).wait_recv()
    finish(last, PART, 0, chunks)
    for chunk in range(chunks - 1):
        swap_sum(blocks + chunk, chunk, 1, last + PART, PART).wait_recv()
        finish(last + PART, PART, chunk, 1)
    for r, (row, size) in enumerate(TAIL):
        swap_sum(blocks + chunks - 1 + r, chunks - 1, 1, last + PART + row, size).wait_recv()
        finish(last + PART + row, size, chunks - 1, 1)
    sent_o.wait_send()
    swap_seen(0, rows).wait_send()
    swap_sum(0, 0, chunks, 0, rows).wait_send()
    swap_y(pl.ds(0, rows), mine).wait_send()
    swap_y(pl.ds(0, rows), theirs).wait_recv()


def solution(mesh):
    def step(x, gain, wq, wk, wv, wo):
        rows, d = x.shape
        heads, kv = wq.shape[1] // HEAD, wk.shape[1] // HEAD
        half = d // 2
        blocks = rows // BQ
        hbm, vmem = pl.BlockSpec(memory_space=pl.ANY), pl.BlockSpec(memory_space=pltpu.VMEM)
        dma = lambda *n: pltpu.SemaphoreType.DMA(n)
        products = 2 * rows * d * (wq.shape[1] + 2 * wk.shape[1]) + 2 * rows * 2 * wo.shape[0] * half
        return pl.pallas_call(
            _kernel,
            out_shape=pltpu.VMEM((rows, d), BF16),
            in_specs=[hbm] * 7,
            out_specs=vmem,
            scratch_shapes=[
                pltpu.VMEM((rows, d), BF16),
                pltpu.VMEM((d,), BF16),
                pltpu.VMEM(wq.shape, BF16),
                pltpu.VMEM(wk.shape, BF16),
                pltpu.VMEM(wv.shape, BF16),
                pltpu.VMEM((2 * wo.shape[0], half), BF16),
                pltpu.VMEM((rows, HEAD), F32),
                pltpu.VMEM((BQ, d), BF16),
                pltpu.VMEM((kv, 2 * BQ, HEAD), BF16),
                pltpu.VMEM((kv, rows, HEAD), BF16),
                pltpu.VMEM((blocks, kv, HEAD + EXTRA, BQ), BF16),
                pltpu.VMEM((8, 2 * BQ), F32),
                pltpu.VMEM((kv, HEAD + EXTRA, 2 * BQ), F32),
                pltpu.VMEM((rows, 2 * heads * HEAD), BF16),
                pltpu.VMEM((half // SPAN, rows, SPAN), BF16),
                pltpu.VMEM((half // SPAN, rows, SPAN), BF16),
                dma(12), dma(half // SPAN + 1), dma(rows // PART), dma(blocks + half // SPAN - 1 + len(TAIL)), dma(4),
            ],
            compiler_params=pltpu.CompilerParams(collective_id=0, has_side_effects=True, vmem_limit_bytes=54 * 2**20),
            cost_estimate=pl.CostEstimate(flops=products + 2 * rows * rows * heads * HEAD, bytes_accessed=40 * 2**20,
                                          transcendentals=rows * rows * heads // 2),
        )(gain, x, wq, wk, wv, wo, jnp.asarray(_rope_table(rows)))

    tokens, columns = P("dp", None), P(None, "tp")
    return jax.shard_map(
        step,
        mesh=mesh,
        in_specs=(tokens, P(None), columns, columns, columns, P("tp", None)),
        out_specs=tokens,
        check_vma=False,
    )
```

```python
import functools

import jax
import jax.numpy as jnp
import numpy as np
from jax import lax
from jax.experimental import pallas as pl
from jax.experimental.pallas import tpu as pltpu
from jax.sharding import PartitionSpec as P

HEAD = 128
THETA = 10000
LOG2E = 1.4426950408889634
HIDDEN = -2e30
BQ = 256
PART = 128
SPAN = 512
TAIL = ((0, 64), (64, 32), (96, 32))
EXTRA = 16
F32, BF16 = jnp.float32, jnp.bfloat16
MESH = pl.DeviceIdType.MESH


def _dot(a, b, ca, cb):
    return lax.dot_general(a, b, (((ca,), (cb,)), ((), ())), preferred_element_type=F32)


def _rope_table(rows):
    half = HEAD // 2
    power = np.float32(THETA) ** (-np.arange(half, dtype=np.float32) / np.float32(half))
    angle = np.arange(rows, dtype=np.float32)[:, None] * power.astype(np.float32)
    return np.concatenate([np.cos(angle), np.sin(angle)], -1).astype(np.float32)


def _kernel(gain_ref, x_ref, wq_ref, wk_ref, wv_ref, wo_ref, tab_ref, y_ref,
            x_s, gain_s, wq_s, wk_s, wv_s, wo_s, tab_s, a_s, q_s, k_s, vt_s, top_s, mix_s, seen_s, sum_s, got_s, wo_e, term_s, got_e, back_s, rest_s,
            in_sem, wo_sem, seen_recv, sum_recv, all_sem, e_sem):
    rows, d = x_s.shape
    kv = k_s.shape[0]
    wide = seen_s.shape[1] // 2
    chunks = sum_s.shape[0]
    half = chunks * SPAN
    blocks, subs, last = rows // BQ, rows // PART, rows - BQ
    e = HEAD**-0.5 * LOG2E
    two = 2 * HEAD
    tp = lax.axis_index("tp")
    core = lax.rem(tp, 2)
    partner = {"tp": tp + 1 - 2 * core}
    peer = {"tp": lax.rem(tp + 2, 4)}
    mine = pl.ds(pl.multiple_of(core * half, half), half)
    theirs = pl.ds(pl.multiple_of((1 - core) * half, half), half)

    def at(start, n):
        return pl.ds(pl.multiple_of(start, min(n, PART)), n)

    barrier = pltpu.get_barrier_semaphore()
    for other in (partner, peer):
        pl.semaphore_signal(barrier, inc=1, device_id=other, device_id_type=MESH)

    def load_x(m):
        edges = (0, PART, BQ, 2 * BQ, rows)
        here = pl.ds(edges[m], edges[m + 1] - edges[m])
        return pltpu.make_async_copy(x_ref.at[here], x_s.at[here], in_sem.at[(0, 1, 2, 3)[m]])

    def load_q(m):
        cols = pl.ds(m * wide // 2, wide // 2)
        return pltpu.make_async_copy(wq_ref.at[:, cols], wq_s.at[:, cols], in_sem.at[2 + m])

    load_k = pltpu.make_async_copy(wk_ref, wk_s, in_sem.at[4])
    load_v = pltpu.make_async_copy(wv_ref, wv_s, in_sem.at[5])
    load_gain = pltpu.make_async_copy(gain_ref, gain_s, in_sem.at[6])
    load_tab = pltpu.make_async_copy(tab_ref.at[:BQ], tab_s.at[:BQ], in_sem.at[7])
    load_rest = pltpu.make_async_copy(tab_ref.at[BQ:], tab_s.at[BQ:], in_sem.at[0])
    load_o = pltpu.make_async_copy(wo_ref.at[:, mine], wo_s.at[:wide], in_sem.at[6])

    load_e = pltpu.make_async_copy(
        wo_ref.at[:, pl.ds(pl.multiple_of((1 - core) * half, half), HEAD)], wo_e, in_sem.at[4])
    swap_o = pltpu.make_async_remote_copy(
        src_ref=wo_ref.at[:, theirs], dst_ref=wo_s.at[wide:], send_sem=wo_sem.at[0], recv_sem=wo_sem.at[1],
        device_id=partner, device_id_type=MESH)


    def swap_seen(m, n=PART):
        here = at(m * PART, n)
        return pltpu.make_async_remote_copy(
            src_ref=seen_s.at[here, :wide], dst_ref=seen_s.at[here, wide:], send_sem=all_sem.at[0], recv_sem=seen_recv.at[lax.rem(m, 2)],
            device_id=partner, device_id_type=MESH)

    def swap_sum(m, first, count, start, n):
        here = at(start, n)
        return pltpu.make_async_remote_copy(
            src_ref=sum_s.at[first : first + count, here], dst_ref=got_s.at[first : first + count, here],
            send_sem=all_sem.at[1], recv_sem=sum_recv.at[m], device_id=peer, device_id_type=MESH)

    swap_term = pltpu.make_async_remote_copy(
        src_ref=term_s, dst_ref=got_e, send_sem=e_sem.at[0], recv_sem=e_sem.at[1], device_id=peer, device_id_type=MESH)
    swap_back = pltpu.make_async_remote_copy(
        src_ref=back_s, dst_ref=rest_s, send_sem=e_sem.at[2], recv_sem=e_sem.at[3], device_id=partner, device_id_type=MESH)

    def swap_first(chunk, left, right):
        cols = pl.ds(left, right - left)
        return pltpu.make_async_remote_copy(
            src_ref=sum_s.at[chunk, :PART, cols], dst_ref=got_s.at[chunk, :PART, cols],
            send_sem=all_sem.at[1], recv_sem=sum_recv.at[0], device_id=peer, device_id_type=MESH)

    def swap_y(here, cols):
        return pltpu.make_async_remote_copy(
            src_ref=y_ref.at[here, cols], dst_ref=y_ref.at[here, cols], send_sem=all_sem.at[2], recv_sem=all_sem.at[3],
            device_id=partner, device_id_type=MESH)

    def norm(start, n):
        gain = gain_s[...].astype(F32).reshape(1, d)
        for m in range(n // 32):
            w = x_s[pl.ds(pl.multiple_of(start + m * 32, 32), 32), :].astype(F32)
            scale = lax.rsqrt(jnp.sum(w * w, -1, keepdims=True) * (1 / d) + 1e-6)
            a_s[m * 32 : (m + 1) * 32, :] = (w * scale * gain).astype(BF16)

    def turn(start, n):
        low = lax.broadcasted_iota(jnp.int32, (n, HEAD), 1) < HEAD // 2
        tab = tab_s[at(start, n), :]
        swapped = pltpu.roll(tab, HEAD // 2, 1)
        cos, sin = jnp.where(low, tab, swapped), jnp.where(low, -swapped, tab)

        def turned(t):
            t = t.astype(BF16).astype(F32)
            return (t * cos + pltpu.roll(t, HEAD // 2, 1) * sin).astype(BF16)

        return turned

    def keys(start, n):
        turned = turn(start, n)
        for h in range(kv // 2):
            t = _dot(a_s[:n, :], wk_s[:, h * two : (h + 1) * two], 1, 0)
            for m in range(2):
                k_s[2 * h + m, at(start, n), :] = turned(t[:, m * HEAD : (m + 1) * HEAD])

    def values(i, off, n):
        for h in range(kv // 2):
            t = _dot(a_s[:n, :], wv_s[:, h * two : (h + 1) * two], 1, 0)
            for m in range(2):
                vt_s[i, 2 * h + m, :HEAD, off : off + n] = t[:, m * HEAD : (m + 1) * HEAD].T.astype(BF16)

    def queries(start, n, heads=None):
        turned = turn(start, n)
        for h in range(kv) if heads is None else heads:
            t = _dot(a_s[:n, :], wq_s[:, h * two : (h + 1) * two], 1, 0)
            for m in range(2):
                q_s[h, m * n : (m + 1) * n, :] = turned(t[:, m * HEAD : (m + 1) * HEAD])

    def attend(i, off, row, stride):
        n, cols, ends = PART, 2 * PART, off + PART

        def scores(h, start, size):
            q = jnp.concatenate([q_s[h, m * stride + row : m * stride + row + n, :] for m in range(2)], axis=0)
            return _dot(k_s[h, at(start, size), :], q, 1, 1)

        gap = lax.rem(lax.broadcasted_iota(jnp.int32, (ends, cols), 1), n) - lax.broadcasted_iota(jnp.int32, (ends, cols), 0)
        weights = []
        for h, s in enumerate([scores(h, i * BQ, ends) for h in range(kv)]):
            s = jnp.where(gap >= -off, s, HIDDEN)
            top = s.max(axis=0, keepdims=True)
            top_s[h : h + 1, :cols] = top
            weights.append(jnp.exp2((s - top) * e).astype(BF16))
        for h, p in enumerate(weights):
            mix_s[h, :, :cols] = _dot(vt_s[i, h, :, :ends], p, 1, 0)

        def whole(j, many):
            weights, keeps = [], []
            for h, s in enumerate([scores(h, j * BQ, many * BQ) for h in range(kv)]):
                old = top_s[h : h + 1, :cols]
                top = jnp.maximum(old, s.max(axis=0, keepdims=True))
                top_s[h : h + 1, :cols] = top
                weights.append(jnp.exp2((s - top) * e).astype(BF16))
                keeps.append(jnp.exp2((old - top) * e))
            for h, (p, keep) in enumerate(zip(weights, keeps)):
                mix = mix_s[h, :, :cols] * keep
                for m in range(many):
                    mix = mix + _dot(vt_s[j + m, h], p[m * BQ : (m + 1) * BQ], 1, 0)
                mix_s[h, :, :cols] = mix

        if not isinstance(i, int):
            lax.fori_loop(0, lax.div(i, 2), lambda j, _: whole(2 * j, 2), None)
            pl.when(lax.rem(i, 2) == 1)(lambda: whole(i - 1, 1))
        for h in range(kv):
            t = (mix_s[h, :HEAD, :cols] * (1 / mix_s[h, HEAD : HEAD + 1, :cols])).T.astype(BF16)
            for m in range(2):
                seen_s[at(i * BQ + off, n), (2 * h + m) * HEAD : (2 * h + m + 1) * HEAD] = t[m * n : (m + 1) * n, :]

    def send(m, chunk):
        if not isinstance(m, int):
            swap_sum(jnp.where(m < subs - 4, 0, 1), chunk, 1, m * PART, PART).start()
        elif m < subs - 1:
            swap_sum(0 if m < subs - 4 else 1 if m < subs - 2 else 2, chunk, 1, m * PART, PART).start()
        elif chunk < chunks - 1:
            swap_sum(3 + chunk, chunk, 1, m * PART, PART).start()
        else:
            for r, (row, size) in enumerate(TAIL):
                swap_sum(2 + chunks + r, chunk, 1, m * PART + row, size).start()

    def give(m):
        here = at(m * PART, PART)
        swap_seen(m).wait_recv()
        for chunk in range(chunks):
            for col in range(0, SPAN, two):
                left = chunk * SPAN + col
                sum_s[chunk, here, col : col + two] = _dot(seen_s[here, :], wo_s[:, left : left + two], 1, 0).astype(BF16)
            send(m, chunk)

    def give_first():
        load_o.wait()
        load_e.wait()
        term_s[...] = _dot(seen_s[:PART, :wide], wo_e[...], 1, 0).astype(BF16)
        mix_s[0, :PART, :two] = _dot(seen_s[:PART, :wide], wo_s[:wide, :two], 1, 0)
        sum_s[0, :PART, :HEAD] = mix_s[0, :PART, :HEAD].astype(BF16)
        swap_first(0, 0, HEAD).start()
        swap_term.start()
        for m in range(1, half // two):
            mix_s[m, :PART, :two] = _dot(seen_s[:PART, :wide], wo_s[:wide, m * two : (m + 1) * two], 1, 0)
        load_x(1).wait()
        norm(PART, PART)
        swap_o.wait_recv()
        swap_seen(0).wait_recv()
        for chunk in range(chunks):
            for col in range(0, SPAN, two):
                m = (chunk * SPAN + col) // two
                t = mix_s[m, :PART, :two] + _dot(seen_s[:PART, wide:], wo_s[wide:, m * two : (m + 1) * two], 1, 0)
                skip = HEAD if m == 0 else 0
                sum_s[chunk, :PART, col + skip : col + two] = t[:, skip:].astype(BF16)
            swap_first(chunk, HEAD if chunk == 0 else 0, SPAN).start()

    load_x(0).start()
    load_gain.start()
    load_tab.start()
    load_k.start()
    load_q(0).start()
    load_q(1).start()
    load_v.start()
    pl.semaphore_wait(barrier, 2)
    swap_o.start()
    load_gain.wait()
    load_x(0).wait()
    norm(0, PART)
    load_tab.wait()
    load_k.wait()
    load_e.start()
    load_o.start()
    load_x(1).start()
    for n in range(blocks):
        vt_s[n, :, HEAD:, :] = jnp.ones((kv, EXTRA, BQ), BF16)
    keys(0, PART)
    load_q(0).wait()
    queries(0, PART, range(kv // 2))
    load_q(1).wait()
    queries(0, PART, range(kv // 2, kv))
    load_v.wait()
    load_x(2).start()
    load_rest.start()
    values(0, 0, PART)
    attend(0, 0, 0, PART)
    swap_seen(0).start()
    load_x(3).start()
    give_first()
    keys(PART, PART)
    values(0, PART, PART)
    queries(PART, PART)
    attend(0, PART, 0, PART)
    swap_seen(1).start()
    load_x(2).wait()
    load_rest.wait()
    norm(BQ, BQ)
    keys(BQ, BQ)
    give(1)
    load_x(3).wait()

    def step(i, _):
        start = i * BQ
        values(i, 0, BQ)
        queries(start, BQ)
        pl.when(i > 1)(lambda: give(2 * i - 1))
        attend(i, 0, 0, BQ)
        swap_seen(2 * i).start()

        @pl.when(i < blocks - 1)
        def _():
            norm(start + BQ, BQ)
            keys(start + BQ, BQ)
            give(2 * i)

        pl.when(i == blocks - 1)(lambda: give(subs - 2))
        attend(i, PART, PART, BQ)
        swap_seen(2 * i + 1).start()

    lax.fori_loop(1, blocks, step, None)
    give(subs - 1)

    def finish(start, n, first, count, rest=False):
        here = at(start, n)
        for chunk in range(first, first + count):
            cols = pl.ds(pl.multiple_of(core * half + chunk * SPAN, SPAN), SPAN)
            both = sum_s[chunk, here, :].astype(F32) + got_s[chunk, here, :].astype(F32)
            if rest and chunk == 0:
                both = jnp.concatenate([both[:, :HEAD] + rest_s[...].astype(F32), both[:, HEAD:]], axis=1)
            y_ref[here, cols] = (x_s[here, cols].astype(F32) + both).astype(BF16)
        swap_y(here, pl.ds(pl.multiple_of(core * half + first * SPAN, SPAN), count * SPAN)).start()

    swap_term.wait_recv()
    back_s[...] = (term_s[...].astype(F32) + got_e[...].astype(F32)).astype(BF16)
    swap_back.start()
    swap_sum(0, 0, chunks, 0, last - BQ).wait_recv()
    finish(PART, PART, 0, chunks)
    lax.fori_loop(1, blocks - 2, lambda i, _: finish(i * BQ, BQ, 0, chunks), None)
    swap_back.wait_recv()
    finish(0, PART, 0, chunks, rest=True)
    swap_sum(1, 0, chunks, last - BQ, BQ).wait_recv()
    finish(last - BQ, BQ, 0, chunks)
    swap_sum(2, 0, chunks, last, PART).wait_recv()
    finish(last, PART, 0, chunks)
    for chunk in range(chunks - 1):
        swap_sum(3 + chunk, chunk, 1, last + PART, PART).wait_recv()
        finish(last + PART, PART, chunk, 1)
    for r, (row, size) in enumerate(TAIL):
        swap_sum(2 + chunks + r, chunks - 1, 1, last + PART + row, size).wait_recv()
        finish(last + PART + row, size, chunks - 1, 1)
    swap_o.wait_send()
    swap_term.wait_send()
    swap_back.wait_send()
    swap_seen(0, rows).wait_send()
    swap_sum(0, 0, chunks, 0, rows).wait_send()
    swap_y(pl.ds(0, rows), mine).wait_send()
    swap_y(pl.ds(0, rows), theirs).wait_recv()


def solution(mesh):
    def step(x, gain, wq, wk, wv, wo):
        rows, d = x.shape
        heads, kv = wq.shape[1] // HEAD, wk.shape[1] // HEAD
        half = d // 2
        blocks = rows // BQ
        hbm, vmem = pl.BlockSpec(memory_space=pl.ANY), pl.BlockSpec(memory_space=pltpu.VMEM)
        dma = lambda *n: pltpu.SemaphoreType.DMA(n)
        products = 2 * rows * d * (wq.shape[1] + 2 * wk.shape[1]) + 2 * rows * 2 * wo.shape[0] * half
        return pl.pallas_call(
            _kernel,
            out_shape=pltpu.VMEM((rows, d), BF16),
            in_specs=[hbm] * 7,
            out_specs=vmem,
            scratch_shapes=[
                pltpu.VMEM((rows, d), BF16),
                pltpu.VMEM((d,), BF16),
                pltpu.VMEM(wq.shape, BF16),
                pltpu.VMEM(wk.shape, BF16),
                pltpu.VMEM(wv.shape, BF16),
                pltpu.VMEM((2 * wo.shape[0], half), BF16),
                pltpu.VMEM((rows, HEAD), F32),
                pltpu.VMEM((BQ, d), BF16),
                pltpu.VMEM((kv, 2 * BQ, HEAD), BF16),
                pltpu.VMEM((kv, rows, HEAD), BF16),
                pltpu.VMEM((blocks, kv, HEAD + EXTRA, BQ), BF16),
                pltpu.VMEM((8, 2 * BQ), F32),
                pltpu.VMEM((kv, HEAD + EXTRA, 2 * BQ), F32),
                pltpu.VMEM((rows, 2 * heads * HEAD), BF16),
                pltpu.VMEM((half // SPAN, rows, SPAN), BF16),
                pltpu.VMEM((half // SPAN, rows, SPAN), BF16),
                pltpu.VMEM((wo.shape[0], HEAD), BF16),
                pltpu.VMEM((PART, HEAD), BF16),
                pltpu.VMEM((PART, HEAD), BF16),
                pltpu.VMEM((PART, HEAD), BF16),
                pltpu.VMEM((PART, HEAD), BF16),
                dma(8), dma(2), dma(2), dma(2 + half // SPAN + len(TAIL)), dma(4), dma(4),
            ],
            compiler_params=pltpu.CompilerParams(collective_id=0, has_side_effects=True, vmem_limit_bytes=54 * 2**20),
            cost_estimate=pl.CostEstimate(flops=products + 2 * rows * rows * heads * HEAD, bytes_accessed=40 * 2**20,
                                          transcendentals=rows * rows * heads // 2),
        )(gain, x, wq, wk, wv, wo, jnp.asarray(_rope_table(rows)))

    tokens, columns = P("dp", None), P(None, "tp")
    return jax.shard_map(
        step,
        mesh=mesh,
        in_specs=(tokens, P(None), columns, columns, columns, P("tp", None)),
        out_specs=tokens,
        check_vma=False,
    )
```

```python
import functools

import jax
import jax.numpy as jnp
import numpy as np
from jax import lax
from jax.experimental import pallas as pl
from jax.experimental.pallas import tpu as pltpu
from jax.sharding import PartitionSpec as P

HEAD = 128
THETA = 10000
LOG2E = 1.4426950408889634
HIDDEN = -2e30
BQ = 256
PART = 128
SPAN = 512
TAIL = ((0, 96), (96, 32))
EXTRA = 16
F32, BF16 = jnp.float32, jnp.bfloat16
MESH = pl.DeviceIdType.MESH


def _dot(a, b, ca, cb):
    return lax.dot_general(a, b, (((ca,), (cb,)), ((), ())), preferred_element_type=F32)


def _rope_table(rows):
    half = HEAD // 2
    power = np.float32(THETA) ** (-np.arange(half, dtype=np.float32) / np.float32(half))
    angle = np.arange(rows, dtype=np.float32)[:, None] * power.astype(np.float32)
    return np.concatenate([np.cos(angle), np.sin(angle)], -1).astype(np.float32)


def _kernel(gain_ref, x_ref, wq_ref, wk_ref, wv_ref, wo_ref, tab_ref, y_ref,
            x_s, gain_s, wq_s, wk_s, wv_s, wo_s, tab_s, a_s, q_s, k_s, vt_s, top_s, mix_s, seen_s, sum_s, got_s, wo_e, term_s, got_e, back_s, rest_s,
            in_sem, wo_sem, seen_recv, sum_recv, all_sem, e_sem):
    rows, d = x_s.shape
    kv = k_s.shape[0]
    wide = seen_s.shape[1] // 2
    chunks = sum_s.shape[0]
    half = chunks * SPAN
    blocks, subs, last = rows // BQ, rows // PART, rows - BQ
    e = HEAD**-0.5 * LOG2E
    two = 2 * HEAD
    tp = lax.axis_index("tp")
    core = lax.rem(tp, 2)
    partner = {"tp": tp + 1 - 2 * core}
    peer = {"tp": lax.rem(tp + 2, 4)}
    mine = pl.ds(pl.multiple_of(core * half, half), half)
    theirs = pl.ds(pl.multiple_of((1 - core) * half, half), half)

    def at(start, n):
        return pl.ds(pl.multiple_of(start, min(n, PART)), n)

    barrier = pltpu.get_barrier_semaphore()
    for other in (partner, peer):
        pl.semaphore_signal(barrier, inc=1, device_id=other, device_id_type=MESH)

    def load_x(m):
        edges = (0, PART, BQ, 2 * BQ, rows)
        here = pl.ds(edges[m], edges[m + 1] - edges[m])
        return pltpu.make_async_copy(x_ref.at[here], x_s.at[here], in_sem.at[(0, 1, 2, 4)[m]])

    def load_w(m):
        ref, to, left = ((wk_ref, wk_s, 0), (wq_ref, wq_s, 0), (wq_ref, wq_s, kv * HEAD), (wv_ref, wv_s, 0))[m // 2]
        here = (pl.ds(m % 2 * (d // 2), d // 2), pl.ds(left, kv * HEAD))
        return pltpu.make_async_copy(ref.at[here], to.at[here], in_sem.at[2 + m])

    load_gain = pltpu.make_async_copy(gain_ref, gain_s, in_sem.at[10])
    load_tab = pltpu.make_async_copy(tab_ref.at[:BQ], tab_s.at[:BQ], in_sem.at[11])
    load_rest = pltpu.make_async_copy(tab_ref.at[BQ:], tab_s.at[BQ:], in_sem.at[0])
    load_o = pltpu.make_async_copy(wo_ref.at[:, mine], wo_s.at[:wide], in_sem.at[12])

    def load_e(m):
        cols = pl.ds(pl.multiple_of(lax.rem(core + m, 2) * half, half), HEAD)
        return pltpu.make_async_copy(wo_ref.at[:, cols], wo_e.at[:, m * HEAD : (m + 1) * HEAD], in_sem.at[13 + m])

    swap_o = pltpu.make_async_remote_copy(
        src_ref=wo_ref.at[:, theirs], dst_ref=wo_s.at[wide:], send_sem=wo_sem.at[0], recv_sem=wo_sem.at[1],
        device_id=partner, device_id_type=MESH)


    def swap_seen(m, n=PART):
        here = at(m * PART, n)
        return pltpu.make_async_remote_copy(
            src_ref=seen_s.at[here, :wide], dst_ref=seen_s.at[here, wide:], send_sem=all_sem.at[0], recv_sem=seen_recv.at[lax.rem(m, 2)],
            device_id=partner, device_id_type=MESH)

    def swap_sum(m, first, count, start, n):
        here = at(start, n)
        return pltpu.make_async_remote_copy(
            src_ref=sum_s.at[first : first + count, here], dst_ref=got_s.at[first : first + count, here],
            send_sem=all_sem.at[1], recv_sem=sum_recv.at[m], device_id=peer, device_id_type=MESH)

    swap_term = pltpu.make_async_remote_copy(
        src_ref=term_s, dst_ref=got_e, send_sem=e_sem.at[0], recv_sem=e_sem.at[1], device_id=peer, device_id_type=MESH)
    swap_back = pltpu.make_async_remote_copy(
        src_ref=back_s, dst_ref=rest_s, send_sem=e_sem.at[2], recv_sem=e_sem.at[3], device_id=partner, device_id_type=MESH)

    def swap_first(chunk, left, right):
        cols = pl.ds(left, right - left)
        return pltpu.make_async_remote_copy(
            src_ref=sum_s.at[chunk, :PART, cols], dst_ref=got_s.at[chunk, :PART, cols],
            send_sem=all_sem.at[1], recv_sem=sum_recv.at[0], device_id=peer, device_id_type=MESH)

    def swap_y(here, cols):
        return pltpu.make_async_remote_copy(
            src_ref=y_ref.at[here, cols], dst_ref=y_ref.at[here, cols], send_sem=all_sem.at[2], recv_sem=all_sem.at[3],
            device_id=partner, device_id_type=MESH)

    def norm(start, n):
        gain = gain_s[...].astype(F32).reshape(1, d)
        for m in range(n // 32):
            w = x_s[pl.ds(pl.multiple_of(start + m * 32, 32), 32), :].astype(F32)
            scale = lax.rsqrt(jnp.sum(w * w, -1, keepdims=True) * (1 / d) + 1e-6)
            a_s[m * 32 : (m + 1) * 32, :] = (w * scale * gain).astype(BF16)

    def turn(start, n):
        low = lax.broadcasted_iota(jnp.int32, (n, HEAD), 1) < HEAD // 2
        tab = tab_s[at(start, n), :]
        swapped = pltpu.roll(tab, HEAD // 2, 1)
        cos, sin = jnp.where(low, tab, swapped), jnp.where(low, -swapped, tab)

        def turned(t):
            t = t.astype(BF16).astype(F32)
            return (t * cos + pltpu.roll(t, HEAD // 2, 1) * sin).astype(BF16)

        return turned

    def product(n, w, h):
        return _dot(a_s[:n, :], w[:, h * two : (h + 1) * two], 1, 0)

    def by_halves(m):
        load_w(m).wait()
        first = (0, 0, kv // 2, 0)[m // 2]
        w = (wk_s, wq_s, wq_s, wv_s)[m // 2]
        for h in range(kv // 2):
            left = (first + h) * two
            mix_s[h, :PART, :two] = _dot(a_s[:PART, : d // 2], w[: d // 2, left : left + two], 1, 0)
        load_w(m + 1).wait()

        def rest(n, w, h):
            return mix_s[h - first, :n, :two] + _dot(a_s[:n, d // 2 :], w[d // 2 :, h * two : (h + 1) * two], 1, 0)

        return rest

    def keys(start, n, product=product):
        turned = turn(start, n)
        for h in range(kv // 2):
            t = product(n, wk_s, h)
            for m in range(2):
                k_s[2 * h + m, at(start, n), :] = turned(t[:, m * HEAD : (m + 1) * HEAD])

    def values(i, off, n, product=product):
        for h in range(kv // 2):
            t = product(n, wv_s, h)
            for m in range(2):
                vt_s[i, 2 * h + m, :HEAD, off : off + n] = t[:, m * HEAD : (m + 1) * HEAD].T.astype(BF16)

    def queries(start, n, heads=None, product=product):
        turned = turn(start, n)
        for h in range(kv) if heads is None else heads:
            t = product(n, wq_s, h)
            for m in range(2):
                q_s[h, m * n : (m + 1) * n, :] = turned(t[:, m * HEAD : (m + 1) * HEAD])

    def attend(i, off, row, stride):
        n, cols, ends = PART, 2 * PART, off + PART

        def scores(h, start, size):
            q = jnp.concatenate([q_s[h, m * stride + row : m * stride + row + n, :] for m in range(2)], axis=0)
            return _dot(k_s[h, at(start, size), :], q, 1, 1)

        gap = lax.rem(lax.broadcasted_iota(jnp.int32, (ends, cols), 1), n) - lax.broadcasted_iota(jnp.int32, (ends, cols), 0)
        weights = []
        for h, s in enumerate([scores(h, i * BQ, ends) for h in range(kv)]):
            s = jnp.where(gap >= -off, s, HIDDEN)
            top = s.max(axis=0, keepdims=True)
            top_s[h : h + 1, :cols] = top
            weights.append(jnp.exp2((s - top) * e).astype(BF16))
        for h, p in enumerate(weights):
            mix_s[h, :, :cols] = _dot(vt_s[i, h, :, :ends], p, 1, 0)

        def whole(j, many):
            weights, keeps = [], []
            for h, s in enumerate([scores(h, j * BQ, many * BQ) for h in range(kv)]):
                old = top_s[h : h + 1, :cols]
                top = jnp.maximum(old, s.max(axis=0, keepdims=True))
                top_s[h : h + 1, :cols] = top
                weights.append(jnp.exp2((s - top) * e).astype(BF16))
                keeps.append(jnp.exp2((old - top) * e))
            for h, (p, keep) in enumerate(zip(weights, keeps)):
                mix = mix_s[h, :, :cols] * keep
                for m in range(many):
                    mix = mix + _dot(vt_s[j + m, h], p[m * BQ : (m + 1) * BQ], 1, 0)
                mix_s[h, :, :cols] = mix

        if not isinstance(i, int):
            lax.fori_loop(0, lax.div(i, 2), lambda j, _: whole(2 * j, 2), None)
            pl.when(lax.rem(i, 2) == 1)(lambda: whole(i - 1, 1))
        for h in range(kv):
            t = (mix_s[h, :HEAD, :cols] * (1 / mix_s[h, HEAD : HEAD + 1, :cols])).T.astype(BF16)
            for m in range(2):
                seen_s[at(i * BQ + off, n), (2 * h + m) * HEAD : (2 * h + m + 1) * HEAD] = t[m * n : (m + 1) * n, :]

    def send(m, chunk):
        if not isinstance(m, int):
            swap_sum(jnp.where(m < subs - 4, 0, 1), chunk, 1, m * PART, PART).start()
        elif m < subs - 1:
            swap_sum(0 if m < subs - 4 else 1 if m < subs - 2 else 2, chunk, 1, m * PART, PART).start()
        elif chunk < chunks - 1:
            swap_sum(3 + chunk, chunk, 1, m * PART, PART).start()
        else:
            for r, (row, size) in enumerate(TAIL):
                swap_sum(2 + chunks + r, chunk, 1, m * PART + row, size).start()

    def give(m):
        here = at(m * PART, PART)
        swap_seen(m).wait_recv()
        for chunk in range(chunks):
            for col in range(0, SPAN, two):
                left = chunk * SPAN + col
                sum_s[chunk, here, col : col + two] = _dot(seen_s[here, :], wo_s[:, left : left + two], 1, 0).astype(BF16)
            send(m, chunk)

    def give_first():
        load_e(0).wait()
        sum_s[0, :PART, :HEAD] = _dot(seen_s[:PART, :wide], wo_e[:, :HEAD], 1, 0).astype(BF16)
        swap_first(0, 0, HEAD).start()
        load_e(1).wait()
        term_s[...] = _dot(seen_s[:PART, :wide], wo_e[:, HEAD:], 1, 0).astype(BF16)
        swap_term.start()
        load_o.wait()
        for m in range(half // two):
            mix_s[m, :PART, :two] = _dot(seen_s[:PART, :wide], wo_s[:wide, m * two : (m + 1) * two], 1, 0)
        load_x(1).wait()
        norm(PART, PART)
        swap_o.wait_recv()
        swap_seen(0).wait_recv()
        for chunk in range(chunks):
            for col in range(0, SPAN, two):
                m = (chunk * SPAN + col) // two
                t = mix_s[m, :PART, :two] + _dot(seen_s[:PART, wide:], wo_s[wide:, m * two : (m + 1) * two], 1, 0)
                skip = HEAD if m == 0 else 0
                sum_s[chunk, :PART, col + skip : col + two] = t[:, skip:].astype(BF16)
            swap_first(chunk, HEAD if chunk == 0 else 0, SPAN).start()

    load_x(0).start()
    load_gain.start()
    load_tab.start()
    for m in range(8):
        load_w(m).start()
    for m in range(2):
        load_e(m).start()
    pl.semaphore_wait(barrier, 2)
    swap_o.start()
    load_gain.wait()
    load_x(0).wait()
    norm(0, PART)
    load_tab.wait()
    load_o.start()
    load_x(1).start()
    keys(0, PART, by_halves(0))
    for n in range(blocks):
        vt_s[n, :, HEAD:, :] = jnp.ones((kv, EXTRA, BQ), BF16)
    queries(0, PART, range(kv // 2), by_halves(2))
    queries(0, PART, range(kv // 2, kv), by_halves(4))
    load_x(2).start()
    load_rest.start()
    values(0, 0, PART, by_halves(6))
    attend(0, 0, 0, PART)
    swap_seen(0).start()
    load_x(3).start()
    give_first()
    keys(PART, PART)
    values(0, PART, PART)
    queries(PART, PART)
    attend(0, PART, 0, PART)
    swap_seen(1).start()
    load_x(2).wait()
    load_rest.wait()
    norm(BQ, BQ)
    keys(BQ, BQ)
    give(1)
    load_x(3).wait()

    def step(i, _):
        start = i * BQ
        values(i, 0, BQ)
        queries(start, BQ)
        pl.when(i > 1)(lambda: give(2 * i - 1))
        attend(i, 0, 0, BQ)
        swap_seen(2 * i).start()

        @pl.when(i < blocks - 1)
        def _():
            norm(start + BQ, BQ)
            keys(start + BQ, BQ)
            give(2 * i)

        pl.when(i == blocks - 1)(lambda: give(subs - 2))
        attend(i, PART, PART, BQ)
        swap_seen(2 * i + 1).start()

    lax.fori_loop(1, blocks, step, None)
    give(subs - 1)

    def finish(start, n, first, count, rest=False):
        here = at(start, n)
        for chunk in range(first, first + count):
            cols = pl.ds(pl.multiple_of(core * half + chunk * SPAN, SPAN), SPAN)
            both = sum_s[chunk, here, :].astype(F32) + got_s[chunk, here, :].astype(F32)
            if rest and chunk == 0:
                both = jnp.concatenate([both[:, :HEAD] + rest_s[...].astype(F32), both[:, HEAD:]], axis=1)
            y_ref[here, cols] = (x_s[here, cols].astype(F32) + both).astype(BF16)
        swap_y(here, pl.ds(pl.multiple_of(core * half + first * SPAN, SPAN), count * SPAN)).start()

    swap_term.wait_recv()
    back_s[...] = (term_s[...].astype(F32) + got_e[...].astype(F32)).astype(BF16)
    swap_back.start()
    swap_sum(0, 0, chunks, 0, last - BQ).wait_recv()
    finish(PART, PART, 0, chunks)
    lax.fori_loop(1, blocks - 2, lambda i, _: finish(i * BQ, BQ, 0, chunks), None)
    swap_back.wait_recv()
    finish(0, PART, 0, chunks, rest=True)
    swap_sum(1, 0, chunks, last - BQ, BQ).wait_recv()
    finish(last - BQ, BQ, 0, chunks)
    swap_sum(2, 0, chunks, last, PART).wait_recv()
    finish(last, PART, 0, chunks)
    for chunk in range(chunks - 1):
        swap_sum(3 + chunk, chunk, 1, last + PART, PART).wait_recv()
        finish(last + PART, PART, chunk, 1)
    for r, (row, size) in enumerate(TAIL):
        swap_sum(2 + chunks + r, chunks - 1, 1, last + PART + row, size).wait_recv()
        finish(last + PART + row, size, chunks - 1, 1)
    swap_o.wait_send()
    swap_term.wait_send()
    swap_back.wait_send()
    swap_seen(0, rows).wait_send()
    swap_sum(0, 0, chunks, 0, rows).wait_send()
    swap_y(pl.ds(0, rows), mine).wait_send()
    swap_y(pl.ds(0, rows), theirs).wait_recv()


def solution(mesh):
    def step(x, gain, wq, wk, wv, wo):
        rows, d = x.shape
        heads, kv = wq.shape[1] // HEAD, wk.shape[1] // HEAD
        half = d // 2
        blocks = rows // BQ
        hbm, vmem = pl.BlockSpec(memory_space=pl.ANY), pl.BlockSpec(memory_space=pltpu.VMEM)
        dma = lambda *n: pltpu.SemaphoreType.DMA(n)
        products = 2 * rows * d * (wq.shape[1] + 2 * wk.shape[1]) + 2 * rows * 2 * wo.shape[0] * half
        return pl.pallas_call(
            _kernel,
            out_shape=pltpu.VMEM((rows, d), BF16),
            in_specs=[hbm] * 7,
            out_specs=vmem,
            scratch_shapes=[
                pltpu.VMEM((rows, d), BF16),
                pltpu.VMEM((d,), BF16),
                pltpu.VMEM(wq.shape, BF16),
                pltpu.VMEM(wk.shape, BF16),
                pltpu.VMEM(wv.shape, BF16),
                pltpu.VMEM((2 * wo.shape[0], half), BF16),
                pltpu.VMEM((rows, HEAD), F32),
                pltpu.VMEM((BQ, d), BF16),
                pltpu.VMEM((kv, 2 * BQ, HEAD), BF16),
                pltpu.VMEM((kv, rows, HEAD), BF16),
                pltpu.VMEM((blocks, kv, HEAD + EXTRA, BQ), BF16),
                pltpu.VMEM((8, 2 * BQ), F32),
                pltpu.VMEM((kv, HEAD + EXTRA, 2 * BQ), F32),
                pltpu.VMEM((rows, 2 * heads * HEAD), BF16),
                pltpu.VMEM((half // SPAN, rows, SPAN), BF16),
                pltpu.VMEM((half // SPAN, rows, SPAN), BF16),
                pltpu.VMEM((wo.shape[0], 2 * HEAD), BF16),
                pltpu.VMEM((PART, HEAD), BF16),
                pltpu.VMEM((PART, HEAD), BF16),
                pltpu.VMEM((PART, HEAD), BF16),
                pltpu.VMEM((PART, HEAD), BF16),
                dma(15), dma(2), dma(2), dma(2 + half // SPAN + len(TAIL)), dma(4), dma(4),
            ],
            compiler_params=pltpu.CompilerParams(collective_id=0, has_side_effects=True, vmem_limit_bytes=54 * 2**20),
            cost_estimate=pl.CostEstimate(flops=products + 2 * rows * rows * heads * HEAD, bytes_accessed=40 * 2**20,
                                          transcendentals=rows * rows * heads // 2),
        )(gain, x, wq, wk, wv, wo, jnp.asarray(_rope_table(rows)))

    tokens, columns = P("dp", None), P(None, "tp")
    return jax.shard_map(
        step,
        mesh=mesh,
        in_specs=(tokens, P(None), columns, columns, columns, P("tp", None)),
        out_specs=tokens,
        check_vma=False,
    )
```

```python
import functools

import jax
import jax.numpy as jnp
import numpy as np
from jax import lax
from jax.experimental import pallas as pl
from jax.experimental.pallas import tpu as pltpu
from jax.sharding import PartitionSpec as P

HEAD = 128
THETA = 10000
LOG2E = 1.4426950408889634
HIDDEN = float("-inf")
BQ = 256
PART = 128
SPAN = 512
TAIL = ((0, 96), (96, 32))
EXTRA = 16
F32, BF16 = jnp.float32, jnp.bfloat16
MESH = pl.DeviceIdType.MESH


def _dot(a, b, ca, cb):
    return lax.dot_general(a, b, (((ca,), (cb,)), ((), ())), preferred_element_type=F32)


def _rope_table(rows):
    half = HEAD // 2
    power = np.float32(THETA) ** (-np.arange(half, dtype=np.float32) / np.float32(half))
    angle = np.arange(rows, dtype=np.float32)[:, None] * power.astype(np.float32)
    return np.concatenate([np.cos(angle), np.sin(angle)], -1).astype(np.float32)


def _kernel(gain_ref, x_ref, wq_ref, wk_ref, wv_ref, wo_ref, tab_ref, y_ref,
            x_s, gain_s, wq_s, wk_s, wv_s, wo_s, tab_s, a_s, q_s, k_s, vt_s, top_s, mix_s, seen_s, sum_s, got_s, wo_e, term_s, got_e, back_s, rest_s,
            in_sem, wo_sem, seen_recv, sum_recv, all_sem, e_sem):
    rows, d = x_s.shape
    kv = k_s.shape[0]
    wide = seen_s.shape[1] // 2
    chunks = sum_s.shape[0]
    half = chunks * SPAN
    blocks, subs, last = rows // BQ, rows // PART, rows - BQ
    e = HEAD**-0.5 * LOG2E
    two = 2 * HEAD
    tp = lax.axis_index("tp")
    core = lax.rem(tp, 2)
    partner = {"tp": tp + 1 - 2 * core}
    peer = {"tp": lax.rem(tp + 2, 4)}
    mine = pl.ds(pl.multiple_of(core * half, half), half)
    theirs = pl.ds(pl.multiple_of((1 - core) * half, half), half)

    def at(start, n):
        return pl.ds(pl.multiple_of(start, min(n, PART)), n)

    barrier = pltpu.get_barrier_semaphore()
    for other in (partner, peer):
        pl.semaphore_signal(barrier, inc=1, device_id=other, device_id_type=MESH)

    def load_x(m):
        edges = (0, PART, BQ, 2 * BQ, rows)
        here = pl.ds(edges[m], edges[m + 1] - edges[m])
        return pltpu.make_async_copy(x_ref.at[here], x_s.at[here], in_sem.at[(0, 1, 2, 4)[m]])

    def load_w(m):
        ref, to, left = ((wk_ref, wk_s, 0), (wq_ref, wq_s, 0), (wq_ref, wq_s, kv * HEAD), (wv_ref, wv_s, 0))[m // 2]
        here = (pl.ds(m % 2 * (d // 2), d // 2), pl.ds(left, kv * HEAD))
        return pltpu.make_async_copy(ref.at[here], to.at[here], in_sem.at[2 + m])

    load_gain = pltpu.make_async_copy(gain_ref, gain_s, in_sem.at[10])
    load_tab = pltpu.make_async_copy(tab_ref.at[:BQ], tab_s.at[:BQ], in_sem.at[11])
    load_rest = pltpu.make_async_copy(tab_ref.at[BQ:], tab_s.at[BQ:], in_sem.at[0])
    load_o = pltpu.make_async_copy(wo_ref.at[:, mine], wo_s.at[:wide], in_sem.at[12])

    load_e = pltpu.make_async_copy(wo_ref.at[:, :two], wo_e, in_sem.at[13])
    swap_o = pltpu.make_async_remote_copy(
        src_ref=wo_ref.at[:, theirs], dst_ref=wo_s.at[wide:], send_sem=wo_sem.at[0], recv_sem=wo_sem.at[1],
        device_id=partner, device_id_type=MESH)


    def swap_seen(m, n=PART):
        here = at(m * PART, n)
        return pltpu.make_async_remote_copy(
            src_ref=seen_s.at[here, :wide], dst_ref=seen_s.at[here, wide:], send_sem=all_sem.at[0], recv_sem=seen_recv.at[lax.rem(m, 2)],
            device_id=partner, device_id_type=MESH)

    def swap_sum(m, first, count, start, n):
        here = at(start, n)
        return pltpu.make_async_remote_copy(
            src_ref=sum_s.at[first : first + count, here], dst_ref=got_s.at[first : first + count, here],
            send_sem=all_sem.at[1], recv_sem=sum_recv.at[m], device_id=peer, device_id_type=MESH)

    swap_term = pltpu.make_async_remote_copy(
        src_ref=term_s, dst_ref=got_e, send_sem=e_sem.at[0], recv_sem=e_sem.at[1], device_id=peer, device_id_type=MESH)
    swap_back = pltpu.make_async_remote_copy(
        src_ref=back_s, dst_ref=rest_s, send_sem=e_sem.at[2], recv_sem=e_sem.at[3], device_id=partner, device_id_type=MESH)

    def swap_first(chunk, left, right):
        cols = pl.ds(left, right - left)
        return pltpu.make_async_remote_copy(
            src_ref=sum_s.at[chunk, :PART, cols], dst_ref=got_s.at[chunk, :PART, cols],
            send_sem=all_sem.at[1], recv_sem=sum_recv.at[0], device_id=peer, device_id_type=MESH)

    def swap_y(here, cols):
        return pltpu.make_async_remote_copy(
            src_ref=y_ref.at[here, cols], dst_ref=y_ref.at[here, cols], send_sem=all_sem.at[2], recv_sem=all_sem.at[3],
            device_id=partner, device_id_type=MESH)

    def norm(start, n):
        gain = gain_s[...].astype(F32).reshape(1, d)
        for m in range(n // 32):
            w = x_s[pl.ds(pl.multiple_of(start + m * 32, 32), 32), :].astype(F32)
            scale = lax.rsqrt(jnp.sum(w * w, -1, keepdims=True) * (1 / d) + 1e-6)
            a_s[m * 32 : (m + 1) * 32, :] = (w * scale * gain).astype(BF16)

    def turn(start, n):
        low = lax.broadcasted_iota(jnp.int32, (n, HEAD), 1) < HEAD // 2
        tab = tab_s[at(start, n), :]
        swapped = pltpu.roll(tab, HEAD // 2, 1)
        cos, sin = jnp.where(low, tab, swapped), jnp.where(low, -swapped, tab)

        def turned(t):
            t = t.astype(BF16).astype(F32)
            return (t * cos + pltpu.roll(t, HEAD // 2, 1) * sin).astype(BF16)

        return turned

    def product(n, w, h):
        return _dot(a_s[:n, :], w[:, h * two : (h + 1) * two], 1, 0)

    def by_halves(m):
        load_w(m).wait()
        first = (0, 0, kv // 2, 0)[m // 2]
        w = (wk_s, wq_s, wq_s, wv_s)[m // 2]
        for h in range(kv // 2):
            left = (first + h) * two
            mix_s[h, :PART, :two] = _dot(a_s[:PART, : d // 2], w[: d // 2, left : left + two], 1, 0)
        load_w(m + 1).wait()

        def rest(n, w, h):
            return mix_s[h - first, :n, :two] + _dot(a_s[:n, d // 2 :], w[d // 2 :, h * two : (h + 1) * two], 1, 0)

        return rest

    def keys(start, n, product=product):
        turned = turn(start, n)
        for h in range(kv // 2):
            t = product(n, wk_s, h)
            for m in range(2):
                k_s[2 * h + m, at(start, n), :] = turned(t[:, m * HEAD : (m + 1) * HEAD])

    def values(i, off, n, product=product):
        for h in range(kv // 2):
            t = product(n, wv_s, h)
            for m in range(2):
                vt_s[i, 2 * h + m, :HEAD, off : off + n] = t[:, m * HEAD : (m + 1) * HEAD].T.astype(BF16)

    def queries(start, n, heads=None, product=product):
        turned = turn(start, n)
        for h in range(kv) if heads is None else heads:
            t = product(n, wq_s, h)
            for m in range(2):
                q_s[h, m * n : (m + 1) * n, :] = turned(t[:, m * HEAD : (m + 1) * HEAD])

    def attend(i, off, row, stride):
        n, cols, ends = PART, 2 * PART, off + PART

        def scores(h, start, size):
            q = jnp.concatenate([q_s[h, m * stride + row : m * stride + row + n, :] for m in range(2)], axis=0)
            return _dot(k_s[h, at(start, size), :], q, 1, 1)

        gap = lax.rem(lax.broadcasted_iota(jnp.int32, (ends, cols), 1), n) - lax.broadcasted_iota(jnp.int32, (ends, cols), 0)
        weights = []
        for h, s in enumerate([scores(h, i * BQ, ends) for h in range(kv)]):
            s = jnp.where(gap >= -off, s, HIDDEN)
            top = s.max(axis=0, keepdims=True)
            top_s[h : h + 1, :cols] = top
            weights.append(jnp.exp2((s - top) * e).astype(BF16))
        for h, p in enumerate(weights):
            mix_s[h, :, :cols] = _dot(vt_s[i, h, :, :ends], p, 1, 0)

        def whole(j, many):
            weights, keeps = [], []
            for h, s in enumerate([scores(h, j * BQ, many * BQ) for h in range(kv)]):
                old = top_s[h : h + 1, :cols]
                top = jnp.maximum(old, s.max(axis=0, keepdims=True))
                top_s[h : h + 1, :cols] = top
                weights.append(jnp.exp2((s - top) * e).astype(BF16))
                keeps.append(jnp.exp2((old - top) * e))
            for h, (p, keep) in enumerate(zip(weights, keeps)):
                mix = mix_s[h, :, :cols] * keep
                for m in range(many):
                    mix = mix + _dot(vt_s[j + m, h], p[m * BQ : (m + 1) * BQ], 1, 0)
                mix_s[h, :, :cols] = mix

        if not isinstance(i, int):
            lax.fori_loop(0, lax.div(i, 2), lambda j, _: whole(2 * j, 2), None)
            pl.when(lax.rem(i, 2) == 1)(lambda: whole(i - 1, 1))
        for h in range(kv):
            t = (mix_s[h, :HEAD, :cols] * (1 / mix_s[h, HEAD : HEAD + 1, :cols])).T.astype(BF16)
            for m in range(2):
                seen_s[at(i * BQ + off, n), (2 * h + m) * HEAD : (2 * h + m + 1) * HEAD] = t[m * n : (m + 1) * n, :]

    def send(m, chunk):
        if not isinstance(m, int):
            swap_sum(jnp.where(m < subs - 4, 0, 1), chunk, 1, m * PART, PART).start()
        elif m < subs - 1:
            swap_sum(0 if m < subs - 4 else 1 if m < subs - 2 else 2, chunk, 1, m * PART, PART).start()
        elif chunk < chunks - 1:
            swap_sum(3 + chunk, chunk, 1, m * PART, PART).start()
        else:
            for r, (row, size) in enumerate(TAIL):
                swap_sum(2 + chunks + r, chunk, 1, m * PART + row, size).start()

    def give(m):
        here = at(m * PART, PART)
        swap_seen(m).wait_recv()
        for chunk in range(chunks):
            for col in range(0, SPAN, two):
                left = chunk * SPAN + col
                sum_s[chunk, here, col : col + two] = _dot(seen_s[here, :], wo_s[:, left : left + two], 1, 0).astype(BF16)
            send(m, chunk)

    def give_first():
        load_e.wait()
        k = pl.ds(0, wide // 2), pl.ds(wide // 2, wide // 2)
        t = _dot(seen_s[:PART, k[0]], wo_e[k[0], :], 1, 0) + _dot(seen_s[:PART, k[1]], wo_e[k[1], :], 1, 0)
        term_s[...] = t.astype(BF16)
        swap_term.start()
        load_o.wait()
        for m in range(half // two):
            mix_s[m, :PART, :two] = _dot(seen_s[:PART, :wide], wo_s[:wide, m * two : (m + 1) * two], 1, 0)
        load_x(1).wait()
        norm(PART, PART)
        swap_o.wait_recv()
        swap_seen(0).wait_recv()
        def column(chunk, col):
            m = (chunk * SPAN + col) // two
            t = mix_s[m, :PART, :two] + _dot(seen_s[:PART, wide:], wo_s[wide:, m * two : (m + 1) * two], 1, 0)
            sum_s[chunk, :PART, col : col + two] = t.astype(BF16)

        for chunk in range(chunks):
            skip = two if chunk == 0 else 0
            for col in range(skip, SPAN, two):
                column(chunk, col)
            swap_first(chunk, skip, SPAN).start()

        @pl.when(core == 1)
        def _():
            column(0, 0)
            swap_first(0, 0, two).start()

    load_x(0).start()
    load_gain.start()
    load_tab.start()
    for m in range(8):
        load_w(m).start()
    load_e.start()
    pl.semaphore_wait(barrier, 2)
    swap_o.start()
    load_gain.wait()
    load_x(0).wait()
    norm(0, PART)
    load_tab.wait()
    load_o.start()
    load_x(1).start()
    keys(0, PART, by_halves(0))
    for n in range(blocks):
        vt_s[n, :, HEAD:, :] = jnp.ones((kv, EXTRA, BQ), BF16)
    queries(0, PART, range(kv // 2), by_halves(2))
    queries(0, PART, range(kv // 2, kv), by_halves(4))
    load_x(2).start()
    load_rest.start()
    values(0, 0, PART, by_halves(6))
    attend(0, 0, 0, PART)
    swap_seen(0).start()
    load_x(3).start()
    give_first()
    keys(PART, PART)
    values(0, PART, PART)
    queries(PART, PART)
    attend(0, PART, 0, PART)
    swap_seen(1).start()
    load_x(2).wait()
    load_rest.wait()
    norm(BQ, BQ)
    keys(BQ, BQ)
    give(1)
    load_x(3).wait()

    def step(i, _):
        start = i * BQ
        values(i, 0, BQ)
        queries(start, BQ)
        pl.when(i > 1)(lambda: give(2 * i - 1))
        attend(i, 0, 0, BQ)
        swap_seen(2 * i).start()

        @pl.when(i < blocks - 1)
        def _():
            norm(start + BQ, BQ)
            keys(start + BQ, BQ)
            give(2 * i)

        pl.when(i == blocks - 1)(lambda: give(subs - 2))
        attend(i, PART, PART, BQ)
        swap_seen(2 * i + 1).start()

    lax.fori_loop(1, blocks, step, None)
    give(subs - 1)

    def finish(start, n, first, count):
        here = at(start, n)
        for chunk in range(first, first + count):
            cols = pl.ds(pl.multiple_of(core * half + chunk * SPAN, SPAN), SPAN)
            both = sum_s[chunk, here, :].astype(F32) + got_s[chunk, here, :].astype(F32)
            y_ref[here, cols] = (x_s[here, cols].astype(F32) + both).astype(BF16)
        swap_y(here, pl.ds(pl.multiple_of(core * half + first * SPAN, SPAN), count * SPAN)).start()

    swap_term.wait()
    short = PART * two // (chunks * SPAN)

    @pl.when(core == 1)
    def _():
        back_s[...] = (term_s[...].astype(F32) + got_e[...].astype(F32)).astype(BF16)
        swap_back.start()
        swap_sum(0, 0, chunks, 0, last - BQ).wait_recv()
        finish(0, PART, 0, 1)
        swap_back.wait_send()

    @pl.when(core == 0)
    def _():
        swap_sum(0, 0, chunks, 0, last - BQ - short).wait_recv()
        swap_back.wait_recv()
        both = term_s[...].astype(F32) + got_e[...].astype(F32) + rest_s[...].astype(F32)
        y_ref[:PART, :two] = (x_s[:PART, :two].astype(F32) + both).astype(BF16)
        left = pl.ds(two, SPAN - two)
        both = sum_s[0, :PART, left].astype(F32) + got_s[0, :PART, left].astype(F32)
        y_ref[:PART, left] = (x_s[:PART, left].astype(F32) + both).astype(BF16)
        swap_y(pl.ds(0, PART), pl.ds(0, SPAN)).start()

    finish(0, PART, 1, chunks - 1)
    finish(PART, PART, 0, chunks)
    lax.fori_loop(1, blocks - 2, lambda i, _: finish(i * BQ, BQ, 0, chunks), None)
    swap_sum(1, 0, chunks, last - BQ, BQ).wait_recv()
    finish(last - BQ, BQ, 0, chunks)
    swap_sum(2, 0, chunks, last, PART).wait_recv()
    finish(last, PART, 0, chunks)
    for chunk in range(chunks - 1):
        swap_sum(3 + chunk, chunk, 1, last + PART, PART).wait_recv()
        finish(last + PART, PART, chunk, 1)
    for r, (row, size) in enumerate(TAIL):
        swap_sum(2 + chunks + r, chunks - 1, 1, last + PART + row, size).wait_recv()
        finish(last + PART + row, size, chunks - 1, 1)
    swap_o.wait_send()
    swap_seen(0, rows).wait_send()
    pl.when(core == 0)(lambda: swap_sum(0, 0, chunks, 0, rows - short).wait_send())
    pl.when(core == 1)(lambda: swap_sum(0, 0, chunks, 0, rows).wait_send())
    swap_y(pl.ds(0, rows), mine).wait_send()
    swap_y(pl.ds(0, rows), theirs).wait_recv()


def solution(mesh):
    def step(x, gain, wq, wk, wv, wo):
        rows, d = x.shape
        heads, kv = wq.shape[1] // HEAD, wk.shape[1] // HEAD
        half = d // 2
        blocks = rows // BQ
        hbm, vmem = pl.BlockSpec(memory_space=pl.ANY), pl.BlockSpec(memory_space=pltpu.VMEM)
        dma = lambda *n: pltpu.SemaphoreType.DMA(n)
        products = 2 * rows * d * (wq.shape[1] + 2 * wk.shape[1]) + 2 * rows * 2 * wo.shape[0] * half
        return pl.pallas_call(
            _kernel,
            out_shape=pltpu.VMEM((rows, d), BF16),
            in_specs=[hbm] * 7,
            out_specs=vmem,
            scratch_shapes=[
                pltpu.VMEM((rows, d), BF16),
                pltpu.VMEM((d,), BF16),
                pltpu.VMEM(wq.shape, BF16),
                pltpu.VMEM(wk.shape, BF16),
                pltpu.VMEM(wv.shape, BF16),
                pltpu.VMEM((2 * wo.shape[0], half), BF16),
                pltpu.VMEM((rows, HEAD), F32),
                pltpu.VMEM((BQ, d), BF16),
                pltpu.VMEM((kv, 2 * BQ, HEAD), BF16),
                pltpu.VMEM((kv, rows, HEAD), BF16),
                pltpu.VMEM((blocks, kv, HEAD + EXTRA, BQ), BF16),
                pltpu.VMEM((8, 2 * BQ), F32),
                pltpu.VMEM((kv, HEAD + EXTRA, 2 * BQ), F32),
                pltpu.VMEM((rows, 2 * heads * HEAD), BF16),
                pltpu.VMEM((half // SPAN, rows, SPAN), BF16),
                pltpu.VMEM((half // SPAN, rows, SPAN), BF16),
                pltpu.VMEM((wo.shape[0], 2 * HEAD), BF16),
                pltpu.VMEM((PART, 2 * HEAD), BF16),
                pltpu.VMEM((PART, 2 * HEAD), BF16),
                pltpu.VMEM((PART, 2 * HEAD), BF16),
                pltpu.VMEM((PART, 2 * HEAD), BF16),
                dma(14), dma(2), dma(2), dma(2 + half // SPAN + len(TAIL)), dma(4), dma(4),
            ],
            compiler_params=pltpu.CompilerParams(collective_id=0, has_side_effects=True, vmem_limit_bytes=54 * 2**20),
            cost_estimate=pl.CostEstimate(flops=products + 2 * rows * rows * heads * HEAD, bytes_accessed=40 * 2**20,
                                          transcendentals=rows * rows * heads // 2),
        )(gain, x, wq, wk, wv, wo, jnp.asarray(_rope_table(rows)))

    tokens, columns = P("dp", None), P(None, "tp")
    return jax.shard_map(
        step,
        mesh=mesh,
        in_specs=(tokens, P(None), columns, columns, columns, P("tp", None)),
        out_specs=tokens,
        check_vma=False,
    )
```

```python
import functools

import jax
import jax.numpy as jnp
import numpy as np
from jax import lax
from jax.experimental import pallas as pl
from jax.experimental.pallas import tpu as pltpu
from jax.sharding import PartitionSpec as P

HEAD = 128
THETA = 10000
LOG2E = 1.4426950408889634
HIDDEN = float("-inf")
BQ = 256
PART = 128
SPAN = 512
TAIL = ((0, 96), (96, 32))
EXTRA = 16
F32, BF16 = jnp.float32, jnp.bfloat16
MESH = pl.DeviceIdType.MESH


def _dot(a, b, ca, cb):
    return lax.dot_general(a, b, (((ca,), (cb,)), ((), ())), preferred_element_type=F32)


def _rope_table(rows):
    half = HEAD // 2
    power = np.float32(THETA) ** (-np.arange(half, dtype=np.float32) / np.float32(half))
    angle = np.arange(rows, dtype=np.float32)[:, None] * power.astype(np.float32)
    return np.concatenate([np.cos(angle), np.sin(angle)], -1).astype(np.float32)


def _kernel(gain_ref, x_ref, wq_ref, wk_ref, wv_ref, wo_ref, tab_ref, y_ref,
            x_s, gain_s, wq_s, wk_s, wv_s, wo_s, tab_s, a_s, q_s, k_s, vt_s, top_s, mix_s, seen_s, sum_s, got_s, wo_e, term_s, got_e, back_s, rest_s,
            in_sem, wo_sem, seen_recv, sum_recv, all_sem, e_sem):
    rows, d = x_s.shape
    kv = k_s.shape[0]
    wide = seen_s.shape[1] // 2
    chunks = sum_s.shape[0]
    half = chunks * SPAN
    blocks, subs, last = rows // BQ, rows // PART, rows - BQ
    e = HEAD**-0.5 * LOG2E
    two = 2 * HEAD
    tp = lax.axis_index("tp")
    core = lax.rem(tp, 2)
    partner = {"tp": tp + 1 - 2 * core}
    peer = {"tp": lax.rem(tp + 2, 4)}
    mine = pl.ds(pl.multiple_of(core * half, half), half)
    theirs = pl.ds(pl.multiple_of((1 - core) * half, half), half)

    def at(start, n):
        return pl.ds(pl.multiple_of(start, min(n, PART)), n)

    barrier = pltpu.get_barrier_semaphore()
    for other in (partner, peer):
        pl.semaphore_signal(barrier, inc=1, device_id=other, device_id_type=MESH)

    def load_x(m):
        edges = (0, PART, BQ, 2 * BQ, rows)
        here = pl.ds(edges[m], edges[m + 1] - edges[m])
        return pltpu.make_async_copy(x_ref.at[here], x_s.at[here], in_sem.at[(0, 11, 2, 4)[m]])

    def load_w(m):
        ref, to, left = ((wk_ref, wk_s, 0), (wq_ref, wq_s, 0), (wq_ref, wq_s, kv * HEAD), (wv_ref, wv_s, 0))[m // 2]
        here = (pl.ds(m % 2 * (d // 2), d // 2), pl.ds(left, kv * HEAD))
        return pltpu.make_async_copy(ref.at[here], to.at[here], in_sem.at[2 + m])

    load_gain = pltpu.make_async_copy(gain_ref, gain_s, in_sem.at[10])
    load_tab = pltpu.make_async_copy(tab_ref.at[:BQ], tab_s.at[:BQ], in_sem.at[11])
    load_rest = pltpu.make_async_copy(tab_ref.at[BQ:], tab_s.at[BQ:], in_sem.at[0])
    load_o = pltpu.make_async_copy(wo_ref.at[:, mine], wo_s.at[:wide], in_sem.at[10])

    load_e = pltpu.make_async_copy(wo_ref.at[:, :two], wo_e, in_sem.at[1])
    swap_o = pltpu.make_async_remote_copy(
        src_ref=wo_ref.at[:, theirs], dst_ref=wo_s.at[wide:], send_sem=wo_sem.at[0], recv_sem=wo_sem.at[1],
        device_id=partner, device_id_type=MESH)


    def swap_seen(m, n=PART):
        here = at(m * PART, n)
        return pltpu.make_async_remote_copy(
            src_ref=seen_s.at[here, :wide], dst_ref=seen_s.at[here, wide:], send_sem=all_sem.at[0], recv_sem=seen_recv.at[lax.rem(m, 2)],
            device_id=partner, device_id_type=MESH)

    def swap_sum(m, first, count, start, n):
        here = at(start, n)
        return pltpu.make_async_remote_copy(
            src_ref=sum_s.at[first : first + count, here], dst_ref=got_s.at[first : first + count, here],
            send_sem=all_sem.at[1], recv_sem=sum_recv.at[m], device_id=peer, device_id_type=MESH)

    swap_term = pltpu.make_async_remote_copy(
        src_ref=term_s, dst_ref=got_e, send_sem=e_sem.at[0], recv_sem=e_sem.at[1], device_id=peer, device_id_type=MESH)
    swap_back = pltpu.make_async_remote_copy(
        src_ref=back_s, dst_ref=rest_s, send_sem=e_sem.at[0], recv_sem=e_sem.at[2], device_id=partner, device_id_type=MESH)

    def swap_first(chunk, left, right):
        cols = pl.ds(left, right - left)
        return pltpu.make_async_remote_copy(
            src_ref=sum_s.at[chunk, :PART, cols], dst_ref=got_s.at[chunk, :PART, cols],
            send_sem=all_sem.at[1], recv_sem=sum_recv.at[0], device_id=peer, device_id_type=MESH)

    def swap_y(here, cols):
        return pltpu.make_async_remote_copy(
            src_ref=y_ref.at[here, cols], dst_ref=y_ref.at[here, cols], send_sem=all_sem.at[2], recv_sem=all_sem.at[3],
            device_id=partner, device_id_type=MESH)

    def norm(start, n):
        gain = gain_s[...].astype(F32).reshape(1, d)
        for m in range(n // 32):
            w = x_s[pl.ds(pl.multiple_of(start + m * 32, 32), 32), :].astype(F32)
            scale = lax.rsqrt(jnp.sum(w * w, -1, keepdims=True) * (1 / d) + 1e-6)
            a_s[m * 32 : (m + 1) * 32, :] = (w * scale * gain).astype(BF16)

    def turn(start, n):
        low = lax.broadcasted_iota(jnp.int32, (n, HEAD), 1) < HEAD // 2
        tab = tab_s[at(start, n), :]
        swapped = pltpu.roll(tab, HEAD // 2, 1)
        cos, sin = jnp.where(low, tab, swapped), jnp.where(low, -swapped, tab)

        def turned(t):
            t = t.astype(BF16).astype(F32)
            return (t * cos + pltpu.roll(t, HEAD // 2, 1) * sin).astype(BF16)

        return turned

    def product(n, w, h):
        return _dot(a_s[:n, :], w[:, h * two : (h + 1) * two], 1, 0)

    def by_halves(m):
        load_w(m).wait()
        first = (0, 0, kv // 2, 0)[m // 2]
        w = (wk_s, wq_s, wq_s, wv_s)[m // 2]
        for h in range(kv // 2):
            left = (first + h) * two
            mix_s[h, :PART, :two] = _dot(a_s[:PART, : d // 2], w[: d // 2, left : left + two], 1, 0)
        load_w(m + 1).wait()

        def rest(n, w, h):
            return mix_s[h - first, :n, :two] + _dot(a_s[:n, d // 2 :], w[d // 2 :, h * two : (h + 1) * two], 1, 0)

        return rest

    def keys(start, n, product=product):
        turned = turn(start, n)
        for h in range(kv // 2):
            t = product(n, wk_s, h)
            for m in range(2):
                k_s[2 * h + m, at(start, n), :] = turned(t[:, m * HEAD : (m + 1) * HEAD])

    def values(i, off, n, product=product):
        for h in range(kv // 2):
            t = product(n, wv_s, h)
            for m in range(2):
                vt_s[i, 2 * h + m, :HEAD, off : off + n] = t[:, m * HEAD : (m + 1) * HEAD].T.astype(BF16)

    def queries(start, n, heads=None, product=product):
        turned = turn(start, n)
        for h in range(kv) if heads is None else heads:
            t = product(n, wq_s, h)
            for m in range(2):
                q_s[h, m * n : (m + 1) * n, :] = turned(t[:, m * HEAD : (m + 1) * HEAD])

    def attend(i, off, row, stride):
        n, cols, ends = PART, 2 * PART, off + PART

        def scores(h, start, size):
            q = jnp.concatenate([q_s[h, m * stride + row : m * stride + row + n, :] for m in range(2)], axis=0)
            return _dot(k_s[h, at(start, size), :], q, 1, 1)

        gap = lax.rem(lax.broadcasted_iota(jnp.int32, (ends, cols), 1), n) - lax.broadcasted_iota(jnp.int32, (ends, cols), 0)
        weights = []
        for h, s in enumerate([scores(h, i * BQ, ends) for h in range(kv)]):
            s = jnp.where(gap >= -off, s, HIDDEN)
            top = s.max(axis=0, keepdims=True)
            top_s[h : h + 1, :cols] = top
            weights.append(jnp.exp2((s - top) * e).astype(BF16))
        for h, p in enumerate(weights):
            mix_s[h, :, :cols] = _dot(vt_s[i, h, :, :ends], p, 1, 0)

        def whole(j, many):
            weights, keeps = [], []
            for h, s in enumerate([scores(h, j * BQ, many * BQ) for h in range(kv)]):
                old = top_s[h : h + 1, :cols]
                top = jnp.maximum(old, s.max(axis=0, keepdims=True))
                top_s[h : h + 1, :cols] = top
                weights.append(jnp.exp2((s - top) * e).astype(BF16))
                keeps.append(jnp.exp2((old - top) * e))
            for h, (p, keep) in enumerate(zip(weights, keeps)):
                mix = mix_s[h, :, :cols] * keep
                for m in range(many):
                    mix = mix + _dot(vt_s[j + m, h], p[m * BQ : (m + 1) * BQ], 1, 0)
                mix_s[h, :, :cols] = mix

        if not isinstance(i, int):
            lax.fori_loop(0, lax.div(i, 2), lambda j, _: whole(2 * j, 2), None)
            pl.when(lax.rem(i, 2) == 1)(lambda: whole(i - 1, 1))
        for h in range(kv):
            t = (mix_s[h, :HEAD, :cols] * (1 / mix_s[h, HEAD : HEAD + 1, :cols])).T.astype(BF16)
            for m in range(2):
                seen_s[at(i * BQ + off, n), (2 * h + m) * HEAD : (2 * h + m + 1) * HEAD] = t[m * n : (m + 1) * n, :]

    def send(m, chunk):
        if not isinstance(m, int):
            swap_sum(jnp.where(m < subs - 4, 0, 1), chunk, 1, m * PART, PART).start()
        elif m < subs - 1:
            swap_sum(0 if m < subs - 4 else 1 if m < subs - 2 else 2, chunk, 1, m * PART, PART).start()
        elif chunk < chunks - 1:
            swap_sum(3 + chunk, chunk, 1, m * PART, PART).start()
        else:
            for r, (row, size) in enumerate(TAIL):
                swap_sum(2 + chunks + r, chunk, 1, m * PART + row, size).start()

    def give(m):
        here = at(m * PART, PART)
        swap_seen(m).wait_recv()
        for chunk in range(chunks):
            for col in range(0, SPAN, two):
                left = chunk * SPAN + col
                sum_s[chunk, here, col : col + two] = _dot(seen_s[here, :], wo_s[:, left : left + two], 1, 0).astype(BF16)
            send(m, chunk)

    def give_first():
        load_e.wait()
        k = pl.ds(0, wide // 2), pl.ds(wide // 2, wide // 2)
        t = _dot(seen_s[:PART, k[0]], wo_e[k[0], :], 1, 0) + _dot(seen_s[:PART, k[1]], wo_e[k[1], :], 1, 0)
        term_s[...] = t.astype(BF16)
        swap_term.start()
        load_o.wait()
        for m in range(half // two):
            mix_s[m, :PART, :two] = _dot(seen_s[:PART, :wide], wo_s[:wide, m * two : (m + 1) * two], 1, 0)
        load_x(1).wait()
        norm(PART, PART)
        swap_o.wait_recv()
        swap_seen(0).wait_recv()
        def column(chunk, col):
            m = (chunk * SPAN + col) // two
            t = mix_s[m, :PART, :two] + _dot(seen_s[:PART, wide:], wo_s[wide:, m * two : (m + 1) * two], 1, 0)
            sum_s[chunk, :PART, col : col + two] = t.astype(BF16)

        for chunk in range(chunks):
            skip = two if chunk == 0 else 0
            for col in range(skip, SPAN, two):
                column(chunk, col)
            swap_first(chunk, skip, SPAN).start()

        @pl.when(core == 1)
        def _():
            column(0, 0)
            swap_first(0, 0, two).start()

    load_x(0).start()
    load_gain.start()
    load_tab.start()
    for m in range(8):
        load_w(m).start()
    load_e.start()
    pl.semaphore_wait(barrier, 2)
    swap_o.start()
    load_gain.wait()
    load_x(0).wait()
    norm(0, PART)
    load_tab.wait()
    load_o.start()
    load_x(1).start()
    keys(0, PART, by_halves(0))
    for n in range(blocks):
        vt_s[n, :, HEAD:, :] = jnp.ones((kv, EXTRA, BQ), BF16)
    queries(0, PART, range(kv // 2), by_halves(2))
    queries(0, PART, range(kv // 2, kv), by_halves(4))
    load_x(2).start()
    load_rest.start()
    values(0, 0, PART, by_halves(6))
    attend(0, 0, 0, PART)
    swap_seen(0).start()
    load_x(3).start()
    give_first()
    keys(PART, PART)
    values(0, PART, PART)
    queries(PART, PART)
    attend(0, PART, 0, PART)
    swap_seen(1).start()
    load_x(2).wait()
    load_rest.wait()
    norm(BQ, BQ)
    keys(BQ, BQ)
    give(1)
    load_x(3).wait()

    def step(i, _):
        start = i * BQ
        values(i, 0, BQ)
        queries(start, BQ)
        pl.when(i > 1)(lambda: give(2 * i - 1))
        attend(i, 0, 0, BQ)
        swap_seen(2 * i).start()

        @pl.when(i < blocks - 1)
        def _():
            norm(start + BQ, BQ)
            keys(start + BQ, BQ)
            give(2 * i)

        pl.when(i == blocks - 1)(lambda: give(subs - 2))
        attend(i, PART, PART, BQ)
        swap_seen(2 * i + 1).start()

    lax.fori_loop(1, blocks, step, None)
    give(subs - 1)

    def finish(start, n, first, count):
        here = at(start, n)
        for chunk in range(first, first + count):
            cols = pl.ds(pl.multiple_of(core * half + chunk * SPAN, SPAN), SPAN)
            both = sum_s[chunk, here, :].astype(F32) + got_s[chunk, here, :].astype(F32)
            y_ref[here, cols] = (x_s[here, cols].astype(F32) + both).astype(BF16)
        swap_y(here, pl.ds(pl.multiple_of(core * half + first * SPAN, SPAN), count * SPAN)).start()

    swap_term.wait()
    short = PART * two // (chunks * SPAN)

    @pl.when(core == 1)
    def _():
        back_s[...] = (term_s[...].astype(F32) + got_e[...].astype(F32)).astype(BF16)
        swap_back.start()
        swap_sum(0, 0, chunks, 0, last - BQ).wait_recv()
        finish(0, PART, 0, 1)
        swap_back.wait_send()

    @pl.when(core == 0)
    def _():
        swap_sum(0, 0, chunks, 0, last - BQ - short).wait_recv()
        swap_back.wait_recv()
        both = term_s[...].astype(F32) + got_e[...].astype(F32) + rest_s[...].astype(F32)
        y_ref[:PART, :two] = (x_s[:PART, :two].astype(F32) + both).astype(BF16)
        left = pl.ds(two, SPAN - two)
        both = sum_s[0, :PART, left].astype(F32) + got_s[0, :PART, left].astype(F32)
        y_ref[:PART, left] = (x_s[:PART, left].astype(F32) + both).astype(BF16)
        swap_y(pl.ds(0, PART), pl.ds(0, SPAN)).start()

    finish(0, PART, 1, chunks - 1)
    finish(PART, PART, 0, chunks)
    lax.fori_loop(1, blocks - 2, lambda i, _: finish(i * BQ, BQ, 0, chunks), None)
    swap_sum(1, 0, chunks, last - BQ, BQ).wait_recv()
    finish(last - BQ, BQ, 0, chunks)
    swap_sum(2, 0, chunks, last, PART).wait_recv()
    finish(last, PART, 0, chunks)
    for chunk in range(chunks - 1):
        swap_sum(3 + chunk, chunk, 1, last + PART, PART).wait_recv()
        finish(last + PART, PART, chunk, 1)
    for r, (row, size) in enumerate(TAIL):
        swap_sum(2 + chunks + r, chunks - 1, 1, last + PART + row, size).wait_recv()
        finish(last + PART + row, size, chunks - 1, 1)
    swap_o.wait_send()
    swap_seen(0, rows).wait_send()
    pl.when(core == 0)(lambda: swap_sum(0, 0, chunks, 0, rows - short).wait_send())
    pl.when(core == 1)(lambda: swap_sum(0, 0, chunks, 0, rows).wait_send())
    swap_y(pl.ds(0, rows), mine).wait_send()
    swap_y(pl.ds(0, rows), theirs).wait_recv()


def solution(mesh):
    def step(x, gain, wq, wk, wv, wo):
        rows, d = x.shape
        heads, kv = wq.shape[1] // HEAD, wk.shape[1] // HEAD
        half = d // 2
        blocks = rows // BQ
        hbm, vmem = pl.BlockSpec(memory_space=pl.ANY), pl.BlockSpec(memory_space=pltpu.VMEM)
        dma = lambda *n: pltpu.SemaphoreType.DMA(n)
        products = 2 * rows * d * (wq.shape[1] + 2 * wk.shape[1]) + 2 * rows * 2 * wo.shape[0] * half
        return pl.pallas_call(
            _kernel,
            out_shape=pltpu.VMEM((rows, d), BF16),
            in_specs=[hbm] * 7,
            out_specs=vmem,
            scratch_shapes=[
                pltpu.VMEM((rows, d), BF16),
                pltpu.VMEM((d,), BF16),
                pltpu.VMEM(wq.shape, BF16),
                pltpu.VMEM(wk.shape, BF16),
                pltpu.VMEM(wv.shape, BF16),
                pltpu.VMEM((2 * wo.shape[0], half), BF16),
                pltpu.VMEM((rows, HEAD), F32),
                pltpu.VMEM((BQ, d), BF16),
                pltpu.VMEM((kv, 2 * BQ, HEAD), BF16),
                pltpu.VMEM((kv, rows, HEAD), BF16),
                pltpu.VMEM((blocks, kv, HEAD + EXTRA, BQ), BF16),
                pltpu.VMEM((8, 2 * BQ), F32),
                pltpu.VMEM((kv, HEAD + EXTRA, 2 * BQ), F32),
                pltpu.VMEM((rows, 2 * heads * HEAD), BF16),
                pltpu.VMEM((half // SPAN, rows, SPAN), BF16),
                pltpu.VMEM((half // SPAN, rows, SPAN), BF16),
                pltpu.VMEM((wo.shape[0], 2 * HEAD), BF16),
                pltpu.VMEM((PART, 2 * HEAD), BF16),
                pltpu.VMEM((PART, 2 * HEAD), BF16),
                pltpu.VMEM((PART, 2 * HEAD), BF16),
                pltpu.VMEM((PART, 2 * HEAD), BF16),
                dma(12), dma(2), dma(2), dma(2 + half // SPAN + len(TAIL)), dma(4), dma(3),
            ],
            compiler_params=pltpu.CompilerParams(collective_id=0, has_side_effects=True, vmem_limit_bytes=54 * 2**20),
            cost_estimate=pl.CostEstimate(flops=products + 2 * rows * rows * heads * HEAD, bytes_accessed=40 * 2**20,
                                          transcendentals=rows * rows * heads // 2),
        )(gain, x, wq, wk, wv, wo, jnp.asarray(_rope_table(rows)))

    tokens, columns = P("dp", None), P(None, "tp")
    return jax.shard_map(
        step,
        mesh=mesh,
        in_specs=(tokens, P(None), columns, columns, columns, P("tp", None)),
        out_specs=tokens,
        check_vma=False,
    )
```

```python
import functools

import jax
import jax.numpy as jnp
import numpy as np
from jax import lax
from jax.experimental import pallas as pl
from jax.experimental.pallas import tpu as pltpu
from jax.sharding import PartitionSpec as P

HEAD = 128
THETA = 10000
LOG2E = 1.4426950408889634
HIDDEN = float("-inf")
BQ = 256
PART = 128
SPAN = 512
TAIL = ((0, 96), (96, 32))
EXTRA = 16
F32, BF16 = jnp.float32, jnp.bfloat16
MESH = pl.DeviceIdType.MESH


def _dot(a, b, ca, cb):
    return lax.dot_general(a, b, (((ca,), (cb,)), ((), ())), preferred_element_type=F32)


def _rope_table(rows):
    half = HEAD // 2
    power = np.float32(THETA) ** (-np.arange(half, dtype=np.float32) / np.float32(half))
    angle = np.arange(rows, dtype=np.float32)[:, None] * power.astype(np.float32)
    return np.concatenate([np.cos(angle), np.sin(angle)], -1).astype(np.float32)


def _kernel(gain_ref, x_ref, wq_ref, wk_ref, wv_ref, wo_ref, tab_ref, y_ref,
            x_s, gain_s, wq_s, wk_s, wv_s, wo_s, tab_s, a_s, q_s, k_s, vt_s, top_s, mix_s, seen_s, sum_s, got_s, wo_e, term_s, got_e, back_s, rest_s,
            in_sem, wo_sem, seen_recv, sum_recv, all_sem, e_sem):
    rows, d = x_s.shape
    kv = k_s.shape[0]
    wide = seen_s.shape[1] // 2
    chunks = sum_s.shape[0]
    half = chunks * SPAN
    blocks, subs, last = rows // BQ, rows // PART, rows - BQ
    e = HEAD**-0.5 * LOG2E
    two = 2 * HEAD
    tp = lax.axis_index("tp")
    core = lax.rem(tp, 2)
    partner = {"tp": tp + 1 - 2 * core}
    peer = {"tp": lax.rem(tp + 2, 4)}
    mine = pl.ds(pl.multiple_of(core * half, half), half)
    theirs = pl.ds(pl.multiple_of((1 - core) * half, half), half)

    def at(start, n):
        return pl.ds(pl.multiple_of(start, min(n, PART)), n)

    barrier = pltpu.get_barrier_semaphore()
    for other in (partner, peer):
        pl.semaphore_signal(barrier, inc=1, device_id=other, device_id_type=MESH)

    def load_x(m):
        edges = (0, PART, BQ, 2 * BQ, rows)
        here = pl.ds(edges[m], edges[m + 1] - edges[m])
        return pltpu.make_async_copy(x_ref.at[here], x_s.at[here], in_sem.at[(0, 11, 2, 4)[m]])

    def load_w(m):
        ref, to, left = ((wk_ref, wk_s, 0), (wq_ref, wq_s, 0), (wq_ref, wq_s, kv * HEAD), (wv_ref, wv_s, 0))[m // 2]
        here = (pl.ds(m % 2 * (d // 2), d // 2), pl.ds(left, kv * HEAD))
        return pltpu.make_async_copy(ref.at[here], to.at[here], in_sem.at[2 + m])

    load_gain = pltpu.make_async_copy(gain_ref, gain_s, in_sem.at[10])
    load_tab = pltpu.make_async_copy(tab_ref.at[:BQ], tab_s.at[:BQ], in_sem.at[11])
    load_rest = pltpu.make_async_copy(tab_ref.at[BQ:], tab_s.at[BQ:], in_sem.at[0])
    load_o = pltpu.make_async_copy(wo_ref.at[:, mine], wo_s.at[:wide], in_sem.at[10])

    load_e = pltpu.make_async_copy(wo_ref.at[:, :two], wo_e, in_sem.at[1])
    swap_o = pltpu.make_async_remote_copy(
        src_ref=wo_ref.at[:, theirs], dst_ref=wo_s.at[wide:], send_sem=wo_sem.at[0], recv_sem=wo_sem.at[1],
        device_id=partner, device_id_type=MESH)


    def swap_seen(m, n=PART):
        here = at(m * PART, n)
        return pltpu.make_async_remote_copy(
            src_ref=seen_s.at[here, :wide], dst_ref=seen_s.at[here, wide:], send_sem=all_sem.at[0], recv_sem=seen_recv.at[lax.rem(m, 2)],
            device_id=partner, device_id_type=MESH)

    def swap_sum(m, first, count, start, n):
        here = at(start, n)
        return pltpu.make_async_remote_copy(
            src_ref=sum_s.at[first : first + count, here], dst_ref=got_s.at[first : first + count, here],
            send_sem=all_sem.at[1], recv_sem=sum_recv.at[m], device_id=peer, device_id_type=MESH)

    swap_term = pltpu.make_async_remote_copy(
        src_ref=term_s, dst_ref=got_e, send_sem=e_sem.at[0], recv_sem=e_sem.at[1], device_id=peer, device_id_type=MESH)
    swap_back = pltpu.make_async_remote_copy(
        src_ref=back_s, dst_ref=rest_s, send_sem=e_sem.at[0], recv_sem=e_sem.at[2], device_id=partner, device_id_type=MESH)

    def swap_first(chunk, left, right):
        cols = pl.ds(left, right - left)
        return pltpu.make_async_remote_copy(
            src_ref=sum_s.at[chunk, :PART, cols], dst_ref=got_s.at[chunk, :PART, cols],
            send_sem=all_sem.at[1], recv_sem=sum_recv.at[0], device_id=peer, device_id_type=MESH)

    def swap_y(here, cols):
        return pltpu.make_async_remote_copy(
            src_ref=y_ref.at[here, cols], dst_ref=y_ref.at[here, cols], send_sem=all_sem.at[2], recv_sem=all_sem.at[3],
            device_id=partner, device_id_type=MESH)

    def norm(start, n):
        gain = gain_s[...].astype(F32).reshape(1, d)
        for m in range(n // 32):
            w = x_s[pl.ds(pl.multiple_of(start + m * 32, 32), 32), :].astype(F32)
            scale = lax.rsqrt(jnp.sum(w * w, -1, keepdims=True) * (1 / d) + 1e-6)
            a_s[m * 32 : (m + 1) * 32, :] = (w * scale * gain).astype(BF16)

    def turn(start, n):
        low = lax.broadcasted_iota(jnp.int32, (n, HEAD), 1) < HEAD // 2
        tab = tab_s[at(start, n), :]
        swapped = pltpu.roll(tab, HEAD // 2, 1)
        cos, sin = jnp.where(low, tab, swapped), jnp.where(low, -swapped, tab)

        def turned(t):
            t = t.astype(BF16).astype(F32)
            return (t * cos + pltpu.roll(t, HEAD // 2, 1) * sin).astype(BF16)

        return turned

    def product(n, w, h):
        return _dot(a_s[:n, :], w[:, h * two : (h + 1) * two], 1, 0)

    def by_halves(m):
        load_w(m).wait()
        first = (0, 0, kv // 2, 0)[m // 2]
        w = (wk_s, wq_s, wq_s, wv_s)[m // 2]
        for h in range(kv // 2):
            left = (first + h) * two
            mix_s[h, :PART, :two] = _dot(a_s[:PART, : d // 2], w[: d // 2, left : left + two], 1, 0)
        load_w(m + 1).wait()

        def rest(n, w, h):
            return mix_s[h - first, :n, :two] + _dot(a_s[:n, d // 2 :], w[d // 2 :, h * two : (h + 1) * two], 1, 0)

        return rest

    def keys(start, n, product=product):
        turned = turn(start, n)
        for h in range(kv // 2):
            t = product(n, wk_s, h)
            for m in range(2):
                k_s[2 * h + m, at(start, n), :] = turned(t[:, m * HEAD : (m + 1) * HEAD])

    def values(i, off, n, product=product):
        for h in range(kv // 2):
            t = product(n, wv_s, h)
            for m in range(2):
                vt_s[i, 2 * h + m, :HEAD, off : off + n] = t[:, m * HEAD : (m + 1) * HEAD].T.astype(BF16)

    def queries(start, n, heads=None, product=product):
        turned = turn(start, n)
        for h in range(kv) if heads is None else heads:
            t = product(n, wq_s, h)
            for m in range(2):
                q_s[h, m * n : (m + 1) * n, :] = turned(t[:, m * HEAD : (m + 1) * HEAD])

    def attend(i, off, row, stride):
        n, cols, ends = PART, 2 * PART, off + PART

        def scores(h, start, size):
            q = jnp.concatenate([q_s[h, m * stride + row : m * stride + row + n, :] for m in range(2)], axis=0)
            return _dot(k_s[h, at(start, size), :], q, 1, 1)

        gap = lax.rem(lax.broadcasted_iota(jnp.int32, (ends, cols), 1), n) - lax.broadcasted_iota(jnp.int32, (ends, cols), 0)
        weights = []
        for h, s in enumerate([scores(h, i * BQ, ends) for h in range(kv)]):
            s = jnp.where(gap >= -off, s, HIDDEN)
            top = s.max(axis=0, keepdims=True)
            top_s[h : h + 1, :cols] = top
            weights.append(jnp.exp2((s - top) * e).astype(BF16))
        for h, p in enumerate(weights):
            mix_s[h, :, :cols] = _dot(vt_s[i, h, :, :ends], p, 1, 0)

        def whole(j, many):
            weights, keeps = [], []
            for h, s in enumerate([scores(h, j * BQ, many * BQ) for h in range(kv)]):
                old = top_s[h : h + 1, :cols]
                top = jnp.maximum(old, s.max(axis=0, keepdims=True))
                top_s[h : h + 1, :cols] = top
                weights.append(jnp.exp2((s - top) * e).astype(BF16))
                keeps.append(jnp.exp2((old - top) * e))
            for h, (p, keep) in enumerate(zip(weights, keeps)):
                mix = mix_s[h, :, :cols] * keep
                for m in range(many):
                    mix = mix + _dot(vt_s[j + m, h], p[m * BQ : (m + 1) * BQ], 1, 0)
                mix_s[h, :, :cols] = mix

        if not isinstance(i, int):
            lax.fori_loop(0, lax.div(i, 2), lambda j, _: whole(2 * j, 2), None)
            pl.when(lax.rem(i, 2) == 1)(lambda: whole(i - 1, 1))
        for h in range(kv):
            t = (mix_s[h, :HEAD, :cols] * (1 / mix_s[h, HEAD : HEAD + 1, :cols])).T.astype(BF16)
            for m in range(2):
                seen_s[at(i * BQ + off, n), (2 * h + m) * HEAD : (2 * h + m + 1) * HEAD] = t[m * n : (m + 1) * n, :]

    def send(m, chunk):
        if not isinstance(m, int):
            swap_sum(jnp.where(m < subs - 4, 0, 1), chunk, 1, m * PART, PART).start()
        elif m < subs - 1:
            swap_sum(0 if m < subs - 4 else 1, chunk, 1, m * PART, PART).start()
        elif chunk < chunks - 1:
            swap_sum(2 + chunk, chunk, 1, m * PART, PART).start()
        else:
            for r, (row, size) in enumerate(TAIL):
                swap_sum(1 + chunks + r, chunk, 1, m * PART + row, size).start()

    def give(m):
        here = at(m * PART, PART)
        swap_seen(m).wait_recv()
        for chunk in range(chunks):
            for col in range(0, SPAN, two):
                left = chunk * SPAN + col
                sum_s[chunk, here, col : col + two] = _dot(seen_s[here, :], wo_s[:, left : left + two], 1, 0).astype(BF16)
            send(m, chunk)

    def give_first():
        load_e.wait()
        k = pl.ds(0, wide // 2), pl.ds(wide // 2, wide // 2)
        t = _dot(seen_s[:PART, k[0]], wo_e[k[0], :], 1, 0) + _dot(seen_s[:PART, k[1]], wo_e[k[1], :], 1, 0)
        term_s[...] = t.astype(BF16)
        swap_term.start()
        load_o.wait()
        for m in range(half // two):
            mix_s[m, :PART, :two] = _dot(seen_s[:PART, :wide], wo_s[:wide, m * two : (m + 1) * two], 1, 0)
        load_x(1).wait()
        norm(PART, PART)
        swap_o.wait_recv()
        swap_seen(0).wait_recv()
        def column(chunk, col):
            m = (chunk * SPAN + col) // two
            t = mix_s[m, :PART, :two] + _dot(seen_s[:PART, wide:], wo_s[wide:, m * two : (m + 1) * two], 1, 0)
            sum_s[chunk, :PART, col : col + two] = t.astype(BF16)

        for chunk in range(chunks):
            skip = two if chunk == 0 else 0
            for col in range(skip, SPAN, two):
                column(chunk, col)
            swap_first(chunk, skip, SPAN).start()

        @pl.when(core == 1)
        def _():
            column(0, 0)
            swap_first(0, 0, two).start()

    load_x(0).start()
    load_gain.start()
    load_tab.start()
    for m in range(8):
        load_w(m).start()
    load_e.start()
    pl.semaphore_wait(barrier, 2)
    swap_o.start()
    load_gain.wait()
    load_x(0).wait()
    norm(0, PART)
    load_tab.wait()
    load_o.start()
    load_x(1).start()
    keys(0, PART, by_halves(0))
    for n in range(blocks):
        vt_s[n, :, HEAD:, :] = jnp.ones((kv, EXTRA, BQ), BF16)
    queries(0, PART, range(kv // 2), by_halves(2))
    queries(0, PART, range(kv // 2, kv), by_halves(4))
    load_x(2).start()
    load_rest.start()
    values(0, 0, PART, by_halves(6))
    attend(0, 0, 0, PART)
    swap_seen(0).start()
    load_x(3).start()
    give_first()
    keys(PART, PART)
    values(0, PART, PART)
    queries(PART, PART)
    attend(0, PART, 0, PART)
    swap_seen(1).start()
    load_x(2).wait()
    load_rest.wait()
    norm(BQ, BQ)
    keys(BQ, BQ)
    give(1)
    load_x(3).wait()

    def step(i, _):
        start = i * BQ
        values(i, 0, BQ)
        queries(start, BQ)
        pl.when(i > 1)(lambda: give(2 * i - 1))
        attend(i, 0, 0, BQ)
        swap_seen(2 * i).start()

        @pl.when(i < blocks - 1)
        def _():
            norm(start + BQ, BQ)
            keys(start + BQ, BQ)
            give(2 * i)

        pl.when(i == blocks - 1)(lambda: give(subs - 2))
        attend(i, PART, PART, BQ)
        swap_seen(2 * i + 1).start()

    lax.fori_loop(1, blocks, step, None)
    give(subs - 1)

    def finish(start, n, first, count):
        here = at(start, n)
        for chunk in range(first, first + count):
            cols = pl.ds(pl.multiple_of(core * half + chunk * SPAN, SPAN), SPAN)
            both = sum_s[chunk, here, :].astype(F32) + got_s[chunk, here, :].astype(F32)
            y_ref[here, cols] = (x_s[here, cols].astype(F32) + both).astype(BF16)
        swap_y(here, pl.ds(pl.multiple_of(core * half + first * SPAN, SPAN), count * SPAN)).start()

    swap_term.wait()
    short = PART * two // (chunks * SPAN)

    @pl.when(core == 1)
    def _():
        back_s[...] = (term_s[...].astype(F32) + got_e[...].astype(F32)).astype(BF16)
        swap_back.start()
        swap_sum(0, 0, chunks, 0, last - BQ).wait_recv()
        finish(0, PART, 0, 1)
        swap_back.wait_send()

    @pl.when(core == 0)
    def _():
        swap_sum(0, 0, chunks, 0, last - BQ - short).wait_recv()
        swap_back.wait_recv()
        both = term_s[...].astype(F32) + got_e[...].astype(F32) + rest_s[...].astype(F32)
        y_ref[:PART, :two] = (x_s[:PART, :two].astype(F32) + both).astype(BF16)
        left = pl.ds(two, SPAN - two)
        both = sum_s[0, :PART, left].astype(F32) + got_s[0, :PART, left].astype(F32)
        y_ref[:PART, left] = (x_s[:PART, left].astype(F32) + both).astype(BF16)
        swap_y(pl.ds(0, PART), pl.ds(0, SPAN)).start()

    finish(0, PART, 1, chunks - 1)
    finish(PART, PART, 0, chunks)
    lax.fori_loop(1, blocks - 2, lambda i, _: finish(i * BQ, BQ, 0, chunks), None)
    swap_sum(1, 0, chunks, last - BQ, BQ + PART).wait_recv()
    finish(last - BQ, BQ, 0, chunks)
    finish(last, PART, 0, chunks)
    for chunk in range(chunks - 1):
        swap_sum(2 + chunk, chunk, 1, last + PART, PART).wait_recv()
        finish(last + PART, PART, chunk, 1)
    for r, (row, size) in enumerate(TAIL):
        swap_sum(1 + chunks + r, chunks - 1, 1, last + PART + row, size).wait_recv()
        finish(last + PART + row, size, chunks - 1, 1)
    swap_o.wait_send()
    swap_seen(0, rows).wait_send()
    pl.when(core == 0)(lambda: swap_sum(0, 0, chunks, 0, rows - short).wait_send())
    pl.when(core == 1)(lambda: swap_sum(0, 0, chunks, 0, rows).wait_send())
    swap_y(pl.ds(0, rows), mine).wait_send()
    swap_y(pl.ds(0, rows), theirs).wait_recv()


def solution(mesh):
    def step(x, gain, wq, wk, wv, wo):
        rows, d = x.shape
        heads, kv = wq.shape[1] // HEAD, wk.shape[1] // HEAD
        half = d // 2
        blocks = rows // BQ
        hbm, vmem = pl.BlockSpec(memory_space=pl.ANY), pl.BlockSpec(memory_space=pltpu.VMEM)
        dma = lambda *n: pltpu.SemaphoreType.DMA(n)
        products = 2 * rows * d * (wq.shape[1] + 2 * wk.shape[1]) + 2 * rows * 2 * wo.shape[0] * half
        return pl.pallas_call(
            _kernel,
            out_shape=pltpu.VMEM((rows, d), BF16),
            in_specs=[hbm] * 7,
            out_specs=vmem,
            scratch_shapes=[
                pltpu.VMEM((rows, d), BF16),
                pltpu.VMEM((d,), BF16),
                pltpu.VMEM(wq.shape, BF16),
                pltpu.VMEM(wk.shape, BF16),
                pltpu.VMEM(wv.shape, BF16),
                pltpu.VMEM((2 * wo.shape[0], half), BF16),
                pltpu.VMEM((rows, HEAD), F32),
                pltpu.VMEM((BQ, d), BF16),
                pltpu.VMEM((kv, 2 * BQ, HEAD), BF16),
                pltpu.VMEM((kv, rows, HEAD), BF16),
                pltpu.VMEM((blocks, kv, HEAD + EXTRA, BQ), BF16),
                pltpu.VMEM((8, 2 * BQ), F32),
                pltpu.VMEM((kv, HEAD + EXTRA, 2 * BQ), F32),
                pltpu.VMEM((rows, 2 * heads * HEAD), BF16),
                pltpu.VMEM((half // SPAN, rows, SPAN), BF16),
                pltpu.VMEM((half // SPAN, rows, SPAN), BF16),
                pltpu.VMEM((wo.shape[0], 2 * HEAD), BF16),
                pltpu.VMEM((PART, 2 * HEAD), BF16),
                pltpu.VMEM((PART, 2 * HEAD), BF16),
                pltpu.VMEM((PART, 2 * HEAD), BF16),
                pltpu.VMEM((PART, 2 * HEAD), BF16),
                dma(12), dma(2), dma(2), dma(1 + half // SPAN + len(TAIL)), dma(4), dma(3),
            ],
            compiler_params=pltpu.CompilerParams(collective_id=0, has_side_effects=True, vmem_limit_bytes=54 * 2**20),
            cost_estimate=pl.CostEstimate(flops=products + 2 * rows * rows * heads * HEAD, bytes_accessed=40 * 2**20,
                                          transcendentals=rows * rows * heads // 2),
        )(gain, x, wq, wk, wv, wo, jnp.asarray(_rope_table(rows)))

    tokens, columns = P("dp", None), P(None, "tp")
    return jax.shard_map(
        step,
        mesh=mesh,
        in_specs=(tokens, P(None), columns, columns, columns, P("tp", None)),
        out_specs=tokens,
        check_vma=False,
    )
```

```python
import functools

import jax
import jax.numpy as jnp
import numpy as np
from jax import lax
from jax.experimental import pallas as pl
from jax.experimental.pallas import tpu as pltpu
from jax.sharding import PartitionSpec as P

HEAD = 128
THETA = 10000
LOG2E = 1.4426950408889634
HIDDEN = float("-inf")
BQ = 256
PART = 128
SPAN = 512
TAIL = ((0, 96), (96, 32))
EXTRA = 16
F32, BF16 = jnp.float32, jnp.bfloat16
MESH = pl.DeviceIdType.MESH


def _dot(a, b, ca, cb):
    return lax.dot_general(a, b, (((ca,), (cb,)), ((), ())), preferred_element_type=F32)


def _rope_table(rows):
    half = HEAD // 2
    power = np.float32(THETA) ** (-np.arange(half, dtype=np.float32) / np.float32(half))
    angle = np.arange(rows, dtype=np.float32)[:, None] * power.astype(np.float32)
    return np.concatenate([np.cos(angle), np.sin(angle)], -1).astype(np.float32)


def _kernel(gain_ref, x_ref, wq_ref, wk_ref, wv_ref, wo_ref, tab_ref, y_ref,
            x_s, gain_s, wq_s, wk_s, wv_s, wo_s, tab_s, a_s, q_s, k_s, vt_s, top_s, mix_s, seen_s, sum_s, got_s, wo_e, term_s, got_e, back_s, rest_s,
            in_sem, wo_sem, seen_recv, sum_recv, all_sem, e_sem):
    rows, d = x_s.shape
    kv = k_s.shape[0]
    wide = seen_s.shape[1] // 2
    chunks = sum_s.shape[0]
    half = chunks * SPAN
    blocks, subs, last = rows // BQ, rows // PART, rows - BQ
    e = HEAD**-0.5 * LOG2E
    two = 2 * HEAD
    tp = lax.axis_index("tp")
    core = lax.rem(tp, 2)
    partner = {"tp": tp + 1 - 2 * core}
    peer = {"tp": lax.rem(tp + 2, 4)}
    mine = pl.ds(pl.multiple_of(core * half, half), half)
    theirs = pl.ds(pl.multiple_of((1 - core) * half, half), half)

    def at(start, n):
        return pl.ds(pl.multiple_of(start, min(n, PART)), n)

    barrier = pltpu.get_barrier_semaphore()
    for other in (partner, peer):
        pl.semaphore_signal(barrier, inc=1, device_id=other, device_id_type=MESH)

    def load_x(m):
        edges = (0, PART, BQ, 2 * BQ, rows)
        here = pl.ds(edges[m], edges[m + 1] - edges[m])
        return pltpu.make_async_copy(x_ref.at[here], x_s.at[here], in_sem.at[(0, 11, 2, 4)[m]])

    def load_w(m):
        ref, to, left = ((wk_ref, wk_s, 0), (wq_ref, wq_s, 0), (wq_ref, wq_s, kv * HEAD), (wv_ref, wv_s, 0))[m // 2]
        here = (pl.ds(m % 2 * (d // 2), d // 2), pl.ds(left, kv * HEAD))
        return pltpu.make_async_copy(ref.at[here], to.at[here], in_sem.at[2 + m])

    load_gain = pltpu.make_async_copy(gain_ref, gain_s, in_sem.at[10])
    load_tab = pltpu.make_async_copy(tab_ref.at[:BQ], tab_s.at[:BQ], in_sem.at[11])
    load_rest = pltpu.make_async_copy(tab_ref.at[BQ:], tab_s.at[BQ:], in_sem.at[0])
    load_o = pltpu.make_async_copy(wo_ref.at[:, mine], wo_s.at[:wide], in_sem.at[10])

    load_e = pltpu.make_async_copy(wo_ref.at[:, :two], wo_e, in_sem.at[1])
    swap_o = pltpu.make_async_remote_copy(
        src_ref=wo_ref.at[:, theirs], dst_ref=wo_s.at[wide:], send_sem=wo_sem.at[0], recv_sem=wo_sem.at[1],
        device_id=partner, device_id_type=MESH)


    def swap_seen(m, n=PART):
        here = at(m * PART, n)
        return pltpu.make_async_remote_copy(
            src_ref=seen_s.at[here, :wide], dst_ref=seen_s.at[here, wide:], send_sem=all_sem.at[0], recv_sem=seen_recv.at[lax.rem(m, 2)],
            device_id=partner, device_id_type=MESH)

    def swap_sum(m, first, count, start, n):
        here = at(start, n)
        return pltpu.make_async_remote_copy(
            src_ref=sum_s.at[first : first + count, here], dst_ref=got_s.at[first : first + count, here],
            send_sem=all_sem.at[1], recv_sem=sum_recv.at[m], device_id=peer, device_id_type=MESH)

    swap_term = pltpu.make_async_remote_copy(
        src_ref=term_s, dst_ref=got_e, send_sem=e_sem.at[0], recv_sem=e_sem.at[1], device_id=peer, device_id_type=MESH)
    swap_back = pltpu.make_async_remote_copy(
        src_ref=back_s, dst_ref=rest_s, send_sem=e_sem.at[0], recv_sem=e_sem.at[2], device_id=partner, device_id_type=MESH)

    def swap_first(chunk, left, right):
        cols = pl.ds(left, right - left)
        return pltpu.make_async_remote_copy(
            src_ref=sum_s.at[chunk, :PART, cols], dst_ref=got_s.at[chunk, :PART, cols],
            send_sem=all_sem.at[1], recv_sem=sum_recv.at[0], device_id=peer, device_id_type=MESH)

    def swap_y(here, cols):
        return pltpu.make_async_remote_copy(
            src_ref=y_ref.at[here, cols], dst_ref=y_ref.at[here, cols], send_sem=all_sem.at[2], recv_sem=all_sem.at[3],
            device_id=partner, device_id_type=MESH)

    def norm(start, n):
        gain = gain_s[...].astype(F32).reshape(1, d)
        for m in range(n // 32):
            w = x_s[pl.ds(pl.multiple_of(start + m * 32, 32), 32), :].astype(F32)
            scale = lax.rsqrt(jnp.sum(w * w, -1, keepdims=True) * (1 / d) + 1e-6)
            a_s[m * 32 : (m + 1) * 32, :] = (w * scale * gain).astype(BF16)

    def turn(start, n):
        low = lax.broadcasted_iota(jnp.int32, (n, HEAD), 1) < HEAD // 2
        tab = tab_s[at(start, n), :]
        swapped = pltpu.roll(tab, HEAD // 2, 1)
        cos, sin = jnp.where(low, tab, swapped), jnp.where(low, -swapped, tab)

        def turned(t):
            t = t.astype(BF16).astype(F32)
            return (t * cos + pltpu.roll(t, HEAD // 2, 1) * sin).astype(BF16)

        return turned

    def product(n, w, h):
        return _dot(a_s[:n, :], w[:, h * two : (h + 1) * two], 1, 0)

    def by_halves(m):
        load_w(m).wait()
        first = (0, 0, kv // 2, 0)[m // 2]
        w = (wk_s, wq_s, wq_s, wv_s)[m // 2]
        for h in range(kv // 2):
            left = (first + h) * two
            mix_s[h, :PART, :two] = _dot(a_s[:PART, : d // 2], w[: d // 2, left : left + two], 1, 0)
        load_w(m + 1).wait()

        def rest(n, w, h):
            return mix_s[h - first, :n, :two] + _dot(a_s[:n, d // 2 :], w[d // 2 :, h * two : (h + 1) * two], 1, 0)

        return rest

    def keys(start, n, product=product):
        turned = turn(start, n)
        for h in range(kv // 2):
            t = product(n, wk_s, h)
            for m in range(2):
                k_s[2 * h + m, at(start, n), :] = turned(t[:, m * HEAD : (m + 1) * HEAD])

    def values(i, off, n, product=product):
        for h in range(kv // 2):
            t = product(n, wv_s, h)
            for m in range(2):
                vt_s[i, 2 * h + m, :HEAD, off : off + n] = t[:, m * HEAD : (m + 1) * HEAD].T.astype(BF16)

    def queries(start, n, heads=None, product=product):
        turned = turn(start, n)
        for h in range(kv) if heads is None else heads:
            t = product(n, wq_s, h)
            for m in range(2):
                q_s[h, m * n : (m + 1) * n, :] = turned(t[:, m * HEAD : (m + 1) * HEAD])

    def attend(i, off, row, stride):
        n, cols, ends = PART, 2 * PART, off + PART

        def scores(h, start, size):
            q = jnp.concatenate([q_s[h, m * stride + row : m * stride + row + n, :] for m in range(2)], axis=0)
            return _dot(k_s[h, at(start, size), :], q, 1, 1)

        gap = lax.rem(lax.broadcasted_iota(jnp.int32, (ends, cols), 1), n) - lax.broadcasted_iota(jnp.int32, (ends, cols), 0)
        weights = []
        for h, s in enumerate([scores(h, i * BQ, ends) for h in range(kv)]):
            s = jnp.where(gap >= -off, s, HIDDEN)
            top = s.max(axis=0, keepdims=True)
            top_s[h : h + 1, :cols] = top
            weights.append(jnp.exp2((s - top) * e).astype(BF16))
        for h, p in enumerate(weights):
            mix_s[h, :, :cols] = _dot(vt_s[i, h, :, :ends], p, 1, 0)

        def whole(j, many):
            weights, keeps = [], []
            for h, s in enumerate([scores(h, j * BQ, many * BQ) for h in range(kv)]):
                old = top_s[h : h + 1, :cols]
                top = jnp.maximum(old, s.max(axis=0, keepdims=True))
                top_s[h : h + 1, :cols] = top
                weights.append(jnp.exp2((s - top) * e).astype(BF16))
                keeps.append(jnp.exp2((old - top) * e))
            for h, (p, keep) in enumerate(zip(weights, keeps)):
                mix = mix_s[h, :, :cols] * keep
                for m in range(many):
                    mix = mix + _dot(vt_s[j + m, h], p[m * BQ : (m + 1) * BQ], 1, 0)
                mix_s[h, :, :cols] = mix

        if not isinstance(i, int):
            lax.fori_loop(0, lax.div(i, 2), lambda j, _: whole(2 * j, 2), None)
            pl.when(lax.rem(i, 2) == 1)(lambda: whole(i - 1, 1))
        for h in range(kv):
            t = (mix_s[h, :HEAD, :cols] * (1 / mix_s[h, HEAD : HEAD + 1, :cols])).T.astype(BF16)
            for m in range(2):
                seen_s[at(i * BQ + off, n), (2 * h + m) * HEAD : (2 * h + m + 1) * HEAD] = t[m * n : (m + 1) * n, :]

    def send(m, chunk):
        if not isinstance(m, int):
            swap_sum(jnp.where(m < subs - 4, 0, 1), chunk, 1, m * PART, PART).start()
        elif m < subs - 1:
            swap_sum(0 if m < subs - 4 else 1, chunk, 1, m * PART, PART).start()
        elif chunk < chunks - 1:
            swap_sum(2 + chunk, chunk, 1, m * PART, PART).start()
        else:
            for r, (row, size) in enumerate(TAIL):
                swap_sum(1 + chunks + r, chunk, 1, m * PART + row, size).start()

    def give(m):
        here = at(m * PART, PART)
        swap_seen(m).wait_recv()
        for chunk in range(chunks):
            for col in range(0, SPAN, two):
                left = chunk * SPAN + col
                sum_s[chunk, here, col : col + two] = _dot(seen_s[here, :], wo_s[:, left : left + two], 1, 0).astype(BF16)
            send(m, chunk)

    def give_first():
        load_e.wait()
        k = pl.ds(0, wide // 2), pl.ds(wide // 2, wide // 2)
        t = _dot(seen_s[:PART, k[0]], wo_e[k[0], :], 1, 0) + _dot(seen_s[:PART, k[1]], wo_e[k[1], :], 1, 0)
        term_s[...] = t.astype(BF16)
        swap_term.start()
        load_o.wait()
        for m in range(half // two):
            mix_s[m, :PART, :two] = _dot(seen_s[:PART, :wide], wo_s[:wide, m * two : (m + 1) * two], 1, 0)
        swap_o.wait_recv()
        swap_seen(0).wait_recv()
        def column(chunk, col):
            m = (chunk * SPAN + col) // two
            t = mix_s[m, :PART, :two] + _dot(seen_s[:PART, wide:], wo_s[wide:, m * two : (m + 1) * two], 1, 0)
            sum_s[chunk, :PART, col : col + two] = t.astype(BF16)

        for chunk in range(chunks):
            skip = two if chunk == 0 else 0
            for col in range(skip, SPAN, two):
                column(chunk, col)
            swap_first(chunk, skip, SPAN).start()

        @pl.when(core == 1)
        def _():
            column(0, 0)
            swap_first(0, 0, two).start()

    load_x(0).start()
    load_gain.start()
    load_tab.start()
    for m in range(8):
        load_w(m).start()
    load_e.start()
    pl.semaphore_wait(barrier, 2)
    swap_o.start()
    load_gain.wait()
    load_x(0).wait()
    norm(0, PART)
    load_tab.wait()
    load_o.start()
    load_x(1).start()
    keys(0, PART, by_halves(0))
    for n in range(blocks):
        vt_s[n, :, HEAD:, :] = jnp.ones((kv, EXTRA, BQ), BF16)
    queries(0, PART, range(kv // 2), by_halves(2))
    queries(0, PART, range(kv // 2, kv), by_halves(4))
    load_x(2).start()
    load_rest.start()
    values(0, 0, PART, by_halves(6))
    attend(0, 0, 0, PART)
    swap_seen(0).start()
    load_x(3).start()
    give_first()
    load_x(1).wait()
    norm(PART, PART)
    keys(PART, PART)
    values(0, PART, PART)
    queries(PART, PART)
    attend(0, PART, 0, PART)
    swap_seen(1).start()
    load_x(2).wait()
    load_rest.wait()
    norm(BQ, BQ)
    keys(BQ, BQ)
    give(1)
    load_x(3).wait()

    def step(i, _):
        start = i * BQ
        values(i, 0, BQ)
        queries(start, BQ)
        pl.when(i > 1)(lambda: give(2 * i - 1))
        attend(i, 0, 0, BQ)
        swap_seen(2 * i).start()

        @pl.when(i < blocks - 1)
        def _():
            norm(start + BQ, BQ)
            keys(start + BQ, BQ)
            give(2 * i)

        pl.when(i == blocks - 1)(lambda: give(subs - 2))
        attend(i, PART, PART, BQ)
        swap_seen(2 * i + 1).start()

    lax.fori_loop(1, blocks, step, None)
    give(subs - 1)

    def finish(start, n, first, count):
        here = at(start, n)
        for chunk in range(first, first + count):
            cols = pl.ds(pl.multiple_of(core * half + chunk * SPAN, SPAN), SPAN)
            both = sum_s[chunk, here, :].astype(F32) + got_s[chunk, here, :].astype(F32)
            y_ref[here, cols] = (x_s[here, cols].astype(F32) + both).astype(BF16)
        swap_y(here, pl.ds(pl.multiple_of(core * half + first * SPAN, SPAN), count * SPAN)).start()

    swap_term.wait()
    short = PART * two // (chunks * SPAN)

    @pl.when(core == 1)
    def _():
        back_s[...] = (term_s[...].astype(F32) + got_e[...].astype(F32)).astype(BF16)
        swap_back.start()
        swap_sum(0, 0, chunks, 0, last - BQ).wait_recv()
        finish(0, PART, 0, 1)
        swap_back.wait_send()

    @pl.when(core == 0)
    def _():
        swap_sum(0, 0, chunks, 0, last - BQ - short).wait_recv()
        swap_back.wait_recv()
        both = term_s[...].astype(F32) + got_e[...].astype(F32) + rest_s[...].astype(F32)
        y_ref[:PART, :two] = (x_s[:PART, :two].astype(F32) + both).astype(BF16)
        left = pl.ds(two, SPAN - two)
        both = sum_s[0, :PART, left].astype(F32) + got_s[0, :PART, left].astype(F32)
        y_ref[:PART, left] = (x_s[:PART, left].astype(F32) + both).astype(BF16)
        swap_y(pl.ds(0, PART), pl.ds(0, SPAN)).start()

    finish(0, PART, 1, chunks - 1)
    finish(PART, PART, 0, chunks)
    lax.fori_loop(1, blocks - 2, lambda i, _: finish(i * BQ, BQ, 0, chunks), None)
    swap_sum(1, 0, chunks, last - BQ, BQ + PART).wait_recv()
    finish(last - BQ, BQ, 0, chunks)
    finish(last, PART, 0, chunks)
    for chunk in range(chunks - 1):
        swap_sum(2 + chunk, chunk, 1, last + PART, PART).wait_recv()
        finish(last + PART, PART, chunk, 1)
    for r, (row, size) in enumerate(TAIL):
        swap_sum(1 + chunks + r, chunks - 1, 1, last + PART + row, size).wait_recv()
        finish(last + PART + row, size, chunks - 1, 1)
    swap_o.wait_send()
    swap_seen(0, rows).wait_send()
    pl.when(core == 0)(lambda: swap_sum(0, 0, chunks, 0, rows - short).wait_send())
    pl.when(core == 1)(lambda: swap_sum(0, 0, chunks, 0, rows).wait_send())
    swap_y(pl.ds(0, rows), mine).wait_send()
    swap_y(pl.ds(0, rows), theirs).wait_recv()


def solution(mesh):
    def step(x, gain, wq, wk, wv, wo):
        rows, d = x.shape
        heads, kv = wq.shape[1] // HEAD, wk.shape[1] // HEAD
        half = d // 2
        blocks = rows // BQ
        hbm, vmem = pl.BlockSpec(memory_space=pl.ANY), pl.BlockSpec(memory_space=pltpu.VMEM)
        dma = lambda *n: pltpu.SemaphoreType.DMA(n)
        products = 2 * rows * d * (wq.shape[1] + 2 * wk.shape[1]) + 2 * rows * 2 * wo.shape[0] * half
        return pl.pallas_call(
            _kernel,
            out_shape=pltpu.VMEM((rows, d), BF16),
            in_specs=[hbm] * 7,
            out_specs=vmem,
            scratch_shapes=[
                pltpu.VMEM((rows, d), BF16),
                pltpu.VMEM((d,), BF16),
                pltpu.VMEM(wq.shape, BF16),
                pltpu.VMEM(wk.shape, BF16),
                pltpu.VMEM(wv.shape, BF16),
                pltpu.VMEM((2 * wo.shape[0], half), BF16),
                pltpu.VMEM((rows, HEAD), F32),
                pltpu.VMEM((BQ, d), BF16),
                pltpu.VMEM((kv, 2 * BQ, HEAD), BF16),
                pltpu.VMEM((kv, rows, HEAD), BF16),
                pltpu.VMEM((blocks, kv, HEAD + EXTRA, BQ), BF16),
                pltpu.VMEM((8, 2 * BQ), F32),
                pltpu.VMEM((kv, HEAD + EXTRA, 2 * BQ), F32),
                pltpu.VMEM((rows, 2 * heads * HEAD), BF16),
                pltpu.VMEM((half // SPAN, rows, SPAN), BF16),
                pltpu.VMEM((half // SPAN, rows, SPAN), BF16),
                pltpu.VMEM((wo.shape[0], 2 * HEAD), BF16),
                pltpu.VMEM((PART, 2 * HEAD), BF16),
                pltpu.VMEM((PART, 2 * HEAD), BF16),
                pltpu.VMEM((PART, 2 * HEAD), BF16),
                pltpu.VMEM((PART, 2 * HEAD), BF16),
                dma(12), dma(2), dma(2), dma(1 + half // SPAN + len(TAIL)), dma(4), dma(3),
            ],
            compiler_params=pltpu.CompilerParams(collective_id=0, has_side_effects=True, vmem_limit_bytes=54 * 2**20),
            cost_estimate=pl.CostEstimate(flops=products + 2 * rows * rows * heads * HEAD, bytes_accessed=40 * 2**20,
                                          transcendentals=rows * rows * heads // 2),
        )(gain, x, wq, wk, wv, wo, jnp.asarray(_rope_table(rows)))

    tokens, columns = P("dp", None), P(None, "tp")
    return jax.shard_map(
        step,
        mesh=mesh,
        in_specs=(tokens, P(None), columns, columns, columns, P("tp", None)),
        out_specs=tokens,
        check_vma=False,
    )
```
